32 devices in a mesh: fsdp: 4 (over y, x), tenant: 4 (over z), dp: 2 (over core).
Axes of the slice: x: 2, y: 2, z: 4, core: 2. Of those that a mesh axis runs over, the one named last changes fastest.
Arguments:
- tokens: bfloat16 [3072, 5120], P(('fsdp', 'dp'), 'tenant'), may hold values from -6 to 6
- block_tenant_index: int32 [48], P(('fsdp', 'dp')), may hold values from 0 to 7
- ranks: int32 [8], replicated, may hold values from 16 to 64, as said below
- frozen_up_weight: bfloat16 [5120, 14336], P(('fsdp', 'dp'), 'tenant'), may hold values from -0.078125 to 0.078125
- tenant_down_adapters: bfloat16 [8, 64, 5120], P('tenant'), may hold values from -0.078125 to 0.078125
- tenant_up_adapters: bfloat16 [8, 64, 14336], P('tenant'), may hold values from -0.75 to 0.75
- cotangent: bfloat16 [3072, 14336], P(('fsdp', 'dp'), 'tenant'), may hold values from -6 to 6
Outputs:
- hidden_out: bfloat16 [3072, 14336], P(('fsdp', 'dp'), 'tenant')
- grad_tokens: bfloat16 [3072, 5120], P(('fsdp', 'dp'), 'tenant')
- grad_down: float32 [8, 64, 5120], P('dp', None, 'tenant')
- grad_up: float32 [8, 64, 14336], P('dp', None, 'tenant')
The draws below stay inside these ranges and needn't reach their ends.
Inputs may be any that keep to these rules, and one draw needn't show every extreme that they name: `ranks`: multiples of 16; some tenant has rank 64.
All inputs are finite; a program needn't handle non-finite values.
Results may differ from the reference program's by a relative error of at most 0.0034.
Values may be sent and summed in bfloat16 or wider, within the bound.
A program may use at most 128 MiB of HBM per device.

```python
import math
import jax
import jax.numpy as jnp
import numpy as np

MODEL_WIDTH = 5120
HIDDEN_UNITS = 14336
TENANT_COUNT = 8
ADAPTER_RANK = 64
BLOCK = 64
TOKENS = 3072
BLOCKS = 48


def draw_ranks(key, part):
    levels = jax.random.randint(key, (TENANT_COUNT,), 1, ADAPTER_RANK // 16 + 1)
    chosen = jax.random.randint(jax.random.fold_in(key, 7), (), 0, TENANT_COUNT)
    levels = jnp.where(jnp.arange(TENANT_COUNT) == chosen, ADAPTER_RANK // 16, levels)
    return (levels * 16).astype(jnp.int32)


def place_ends(drawn, key, least, high):
    place = [jax.random.randint(jax.random.fold_in(key, axis), (), 0, length) for axis, length in enumerate(drawn.shape)]
    main_axis = drawn.shape.index(max(drawn.shape))
    next_to = place[:main_axis] + [(place[main_axis] + 1) % drawn.shape[main_axis]] + place[main_axis + 1:]
    return drawn.at[tuple(place)].set(least).at[tuple(next_to)].set(high)


def shard_levels(key, extent, shards, smallest, top_value):
    factor_of = 1.0
    for dim, blocks in shards:
        steps = jax.random.uniform(jax.random.fold_in(jax.random.fold_in(key, 6), dim), (blocks,), jnp.float32, smallest / len(shards), top_value / len(shards))
        factor_of = factor_of * jnp.repeat(jnp.exp(steps), extent[dim] // blocks).reshape((-1,) + (1,) * (len(extent) - 1 - dim))
    return factor_of


def rank_table(number_of, lean):
    weights = [(1 << 20) // math.isqrt(grade ** lean) + 1 for grade in range(1, number_of + 1)]
    deviation = 1 + sum(weights) // (1 << 30)
    return np.cumsum(np.array([max(1, weight // deviation) for weight in weights]))


def ranked(stream_key, extent, number_of, skew):
    grid = rank_table(number_of, skew)
    pick = jax.random.randint(jax.random.fold_in(stream_key, 1), extent, 0, int(grid[number_of - 1]))
    rank = jnp.searchsorted(jnp.asarray(grid, jnp.int32), pick, side="right")
    return jax.random.permutation(jax.random.fold_in(stream_key, 2), number_of)[rank].astype(jnp.int32)


def centred(stream_key, extent, spread, most, shards=(), kind=jnp.bfloat16):
    result = spread * jax.random.normal(stream_key, extent, jnp.float32)
    if shards:
        result = result * shard_levels(stream_key, extent, shards, -0.22, 0.18)
    return jnp.clip(result, -most, most).astype(kind)


def setup_inputs(seed: int = 0) -> dict:
    splits = jax.random.split(jax.random.key(seed), 8)
    return {
        "tokens": centred(splits[0], (TOKENS, MODEL_WIDTH), 1.0, 6.0, ((0, 8), (1, 4))),
        "block_tenant_index": place_ends(ranked(splits[1], (BLOCKS,), TENANT_COUNT, 2), jax.random.fold_in(splits[1], 3), 0, TENANT_COUNT - 1).astype(jnp.int32),
        "ranks": draw_ranks(jax.random.fold_in(splits[7], 71), 0),
        "frozen_up_weight": centred(splits[3], (MODEL_WIDTH, HIDDEN_UNITS), MODEL_WIDTH ** -0.5, 0.078125, ((0, 8), (1, 4))),
        "tenant_down_adapters": centred(splits[4], (TENANT_COUNT, ADAPTER_RANK, MODEL_WIDTH), MODEL_WIDTH ** -0.5, 0.078125, ((0, 4),)),
        "tenant_up_adapters": centred(splits[5], (TENANT_COUNT, ADAPTER_RANK, HIDDEN_UNITS), ADAPTER_RANK ** -0.5, 0.75, ((0, 4),)),
        "cotangent": centred(splits[6], (TOKENS, HIDDEN_UNITS), 1.0, 6.0, ((0, 8), (1, 4))),
    }


alpha_scale = 32.0


def make_gain(block_tenant_index, ranks):
    rows_tenant = jnp.repeat(block_tenant_index, BLOCK, total_repeat_length=TOKENS)
    columns = jnp.arange(TENANT_COUNT * ADAPTER_RANK, dtype=jnp.int32)
    col_tenant = columns // ADAPTER_RANK
    col_slot = columns % ADAPTER_RANK
    ranks_col = jnp.repeat(ranks, ADAPTER_RANK, total_repeat_length=TENANT_COUNT * ADAPTER_RANK)
    keep = (rows_tenant[:, None] == col_tenant[None, :]) & (col_slot[None, :] < ranks_col[None, :])
    scale_col = alpha_scale / ranks_col.astype(jnp.float32)
    return jnp.where(keep, scale_col[None, :], jnp.float32(0.0))


def reference(tokens, block_tenant_index, ranks, frozen_up_weight, tenant_down_adapters, tenant_up_adapters, cotangent):
    gain = make_gain(block_tenant_index, ranks)
    flattened_down = tenant_down_adapters.reshape(TENANT_COUNT * ADAPTER_RANK, MODEL_WIDTH)
    flattened_up = tenant_up_adapters.reshape(TENANT_COUNT * ADAPTER_RANK, HIDDEN_UNITS)
    proj = jnp.dot(tokens, flattened_down.T, preferred_element_type=jnp.float32)
    adapted = (proj * gain).astype(jnp.bfloat16)
    base = jnp.dot(tokens, frozen_up_weight, preferred_element_type=jnp.float32)
    hidden_out = (base + jnp.dot(adapted, flattened_up, preferred_element_type=jnp.float32)).astype(jnp.bfloat16)
    back = jnp.dot(cotangent, flattened_up.T, preferred_element_type=jnp.float32)
    adapted_grad = (back * gain).astype(jnp.bfloat16)
    grad_base = jnp.dot(cotangent, frozen_up_weight.T, preferred_element_type=jnp.float32)
    grad_tokens = (grad_base + jnp.dot(adapted_grad, flattened_down, preferred_element_type=jnp.float32)).astype(jnp.bfloat16)
    grad_up = jnp.dot(adapted.T, cotangent, preferred_element_type=jnp.float32).reshape(TENANT_COUNT, ADAPTER_RANK, HIDDEN_UNITS)
    grad_down = jnp.dot(adapted_grad.T, tokens, preferred_element_type=jnp.float32).reshape(TENANT_COUNT, ADAPTER_RANK, MODEL_WIDTH)
    return hidden_out, grad_tokens, grad_down, grad_up
```

```python
import functools
import math

import jax
import jax.numpy as jnp
import numpy as np
from jax import lax
from jax.experimental import pallas as pl
from jax.experimental.pallas import tpu as pltpu
from jax.sharding import PartitionSpec as P

BLOCK = 64
PIECES = 5

alpha_scale = 32.0

BF16 = jnp.bfloat16
F32 = jnp.float32
MESH = pl.DeviceIdType.MESH


def nt(a, b):
    return lax.dot_general(a, b, (((1,), (1,)), ((), ())), preferred_element_type=F32)


def tn(a, b):
    return lax.dot_general(a, b, (((0,), (0,)), ((), ())), preferred_element_type=F32)


def nn(a, b):
    return jnp.dot(a, b, preferred_element_type=F32)


def tile_of(width, most=512):
    return max(t for t in range(128, most + 1, 128) if width % t == 0)


def snake(i, n):
    side = math.isqrt(n)
    if side * side != n:
        return i
    row, col = i // side, i % side
    odd = row % 2
    return row * side + (1 - odd) * col + odd * (side - 1 - col)


def kernel(n, m, tenants_of, ranks, tokens, split, cot, w, dn, up, eye,
           hid_o, gt_o, gr_o,
           wbuf, cotv, tokv, tv, hid, upv, dnv, part, come, gp, dpr, rsr, ags, sums, ada, adg,
           l_sem, ws, wr, os, orr, ds, dr, ts, tr, as_, ar, xs, xr, ss, sr, gs, gr, ps, pr, rs, rr, qs, qr, o_sem, cred):
    f, z, c = lax.axis_index("fsdp"), lax.axis_index("tenant"), lax.axis_index("dp")
    rows, ld = tokens.shape
    lf = cot.shape[1]
    depth = w.shape[0]
    piece = depth // PIECES
    own, rank, _ = dn.shape
    tenants = ranks.shape[0]
    half = n // 2
    share = rank // 2
    quarter = gp.shape[0] // n
    blocks = rows // BLOCK
    tile = tile_of(lf)
    aligned = depth % 128 == 0

    place = snake(f, n)
    right, left = snake((place + 1) % n, n), snake((place + n - 1) % n, n)
    to_right, to_left, partner = (right, z, c), (left, z, c), (f, z, 1 - c)

    def plane(t):
        return (f, t, c)

    def owner(s):
        return snake((place + n - s) % n, n)

    def phys(s):
        return 0 if s in (0, half) else s if s < half else s - 1

    def rcopy(src, dst, send, recv, device):
        return pltpu.make_async_remote_copy(
            src_ref=src, dst_ref=dst, send_sem=send, recv_sem=recv, device_id=device, device_id_type=MESH
        )

    sent = []

    def start(copy, cond=None):
        if cond is None:
            copy.start()
        else:
            pl.when(cond)(copy.start)
        sent.append((cond, copy))

    barrier = pltpu.get_barrier_semaphore()
    for k in range(1, n):
        pl.semaphore_signal(barrier, inc=1, device_id=(snake((place + k) % n, n), z, c), device_id_type=MESH)
    for k in range(1, m):
        pl.semaphore_signal(barrier, inc=1, device_id=plane((z + k) % m), device_id_type=MESH)
    pl.semaphore_signal(barrier, inc=1, device_id=partner, device_id_type=MESH)

    def tok_src(ca):
        return tokens.at[:, ca * depth:(ca + 1) * depth] if aligned else split.at[ca]

    local = [
        pltpu.make_async_copy(w.reshape(PIECES, piece, lf), wbuf.at[0, 0], l_sem.at[0]),
        pltpu.make_async_copy(cot, cotv, l_sem.at[1]),
        pltpu.make_async_copy(tokens, tokv, l_sem.at[2]),
        pltpu.make_async_copy(tok_src(0), tv.at[z, 0], l_sem.at[3]),
        pltpu.make_async_copy(tok_src(1), tv.at[z, 1], l_sem.at[4]),
        pltpu.make_async_copy(
            dn.at[:, :, pl.ds(pl.multiple_of(z * ld, 128), ld)], dnv.at[pl.ds(z * own, own)], l_sem.at[5]),
        pltpu.make_async_copy(
            up.at[:, :, pl.ds(pl.multiple_of(z * lf, 128), lf)], upv.at[pl.ds(z * own, own)], l_sem.at[6]),
    ]
    for copy in local:
        copy.start()
    pl.semaphore_wait(barrier, n + m - 1)

    pieces = w.reshape(PIECES, piece, lf)
    for i in range(PIECES):
        a, b = i, PIECES - 1 - i
        start(rcopy(pieces.at[a], wbuf.at[0, phys(1), a], ws.at[0, 0, a], wr.at[0, 0, a], to_right))
        start(rcopy(pieces.at[b], wbuf.at[0, phys(n - 1), b], ws.at[0, 1, b], wr.at[0, 1, b], to_left))
    start(rcopy(pieces, wbuf.at[1, 0], os.at[0], orr.at[0], partner))

    for ca in range(2):
        start(rcopy(tok_src(ca), tv.at[z, ca], ts.at[0, 0, ca], tr.at[z, ca], plane(z + 1)), z < m - 1)
        start(rcopy(tok_src(ca), tv.at[z, ca], ts.at[0, 1, ca], tr.at[z, ca], plane(z - 1)), z > 0)

    def send_adapters(way, cond):
        step = 1 if way == 0 else -1
        mine = pl.ds(pl.multiple_of(c * share, 16), share)
        for j in range(1, m):
            t = z + step * j
            inside = cond & ((t < m) if way == 0 else (t >= 0))
            for kind, (src, dst, width) in enumerate(((dn, dnv, ld), (up, upv, lf))):
                start(rcopy(
                    src.at[:, mine, pl.ds(pl.multiple_of(t * width, 128), width)],
                    dst.at[pl.ds(z * own, own), mine],
                    as_.at[way, j - 1, kind], ar.at[way, j - 1, kind], plane(t)), inside)

    def hop(s, cc):
        d = owner(s)
        upward = (d > z).astype(jnp.int32)
        t = z + 2 * upward - 1
        last_down = (1 - upward) * (t == d).astype(jnp.int32)
        slot = s + (n - s) * last_down
        return rcopy(part.at[s, cc], come.at[slot, cc], gs.at[s, cc], gr.at[slot, cc], plane(t))

    def product(s, cc, ph):
        d = owner(s)
        block = wbuf[cc, ph].reshape(depth, lf)
        part[s, cc] = nt(cotv[...], block).astype(BF16)
        pl.when(((d > z) & (z == 0)) | ((d < z) & (z == m - 1)))(hop(s, cc).start)

    def combine(s, cc, pos):
        d = owner(s)

        @pl.when(((d > z) & (z == pos)) | ((d < z) & (m - 1 - z == pos)))
        def _():
            rcopy(part.at[s, cc], come.at[s, cc], gs.at[s, cc], gr.at[s, cc], partner).wait_recv()
            part[s, cc] = (part[s, cc].astype(F32) + come[s, cc].astype(F32)).astype(BF16)
            hop(s, cc).start()

    def combine_all(first, count, pos):
        @pl.loop(0, 2 * count)
        def _(i):
            k = i // 2
            s = first + k + (k // (half - 1)) * (1 if first else 0)
            combine(s, i % 2, pos)

    local[0].wait()
    local[1].wait()

    product(0, 0, 0)
    rcopy(pieces, wbuf.at[1, 0], os.at[0], orr.at[0], partner).wait_recv()
    product(0, 1, 0)

    send_adapters(0, z == 0)
    send_adapters(1, z == m - 1)
    for k in range(1, m):
        for way, t, there in ((0, z - k, z - k >= 0), (1, z + k, z + k < m)):
            nxt = z + 1 if way == 0 else z - 1
            more = there & ((nxt < m) if way == 0 else (nxt >= 0))
            for ca in range(2):
                pl.when(there)(rcopy(
                    tv.at[t, ca], tv.at[t, ca], ts.at[0, 0, ca], tr.at[t, ca], partner).wait_recv)
                if k < m - 1:
                    start(rcopy(tv.at[t, ca], tv.at[t, ca], ts.at[k, way, ca], tr.at[t, ca], plane(nxt)), more)
        send_adapters(0, z == k)
        send_adapters(1, m - 1 - z == k)

    for copy in local[2:]:
        copy.wait()

    def feature(s, cc):
        core = c if cc == 0 else 1 - c
        return tv[owner(s), core]

    def forward(spots, body):
        @pl.loop(0, lf // tile)
        def _(j):
            columns = pl.ds(pl.multiple_of(j * tile, tile), tile)
            total = None
            for s, cc in spots:
                block = wbuf[cc, phys(s), :, :, columns].reshape(depth, tile)
                term = nn(feature(s, cc), block)
                total = term if total is None else total + term
            body(columns, total)

    def set_hid(columns, total):
        hid[:, columns] = total

    def add_hid(columns, total):
        hid[:, columns] += total

    forward(((0, 0), (0, 1)), set_hid)
    pl.semaphore_signal(cred.at[0], inc=1, device_id=to_left, device_id_type=MESH)
    pl.semaphore_signal(cred.at[1], inc=1, device_id=to_right, device_id_type=MESH)
    pl.semaphore_signal(cred.at[2], inc=1, device_id=partner, device_id_type=MESH)

    pl.semaphore_wait(cred.at[0], 1)
    pl.semaphore_wait(cred.at[1], 1)

    def arrived(stage, way, i, ph):
        rcopy(wbuf.at[0, ph, i], wbuf.at[0, ph, i], ws.at[stage, way, i], wr.at[stage, way, i], partner).wait_recv()

    def across(s, i):
        start(rcopy(wbuf.at[0, phys(s), i], wbuf.at[1, phys(s), i], ds.at[s, i], dr.at[s, i], partner))

    mid = PIECES // 2
    for stage in range(half - 1):
        last = stage == half - 2
        for i in range(PIECES):
            for way in range(2):
                q = i if way == 0 else PIECES - 1 - i
                s = stage + 1 if way == 0 else n - stage - 1
                arrived(stage, way, q, phys(s))
                on = stage + 2 if way == 0 else n - stage - 2
                if not last or i < mid:
                    start(rcopy(wbuf.at[0, phys(s), q], wbuf.at[0, phys(on), q], ws.at[stage + 1, way, q],
                                wr.at[stage + 1, way, q], to_right if way == 0 else to_left))
                across(s, q)
            if last and i == mid:
                ph = phys(half - 1) * (1 - c) + phys(half + 1) * c
                start(rcopy(wbuf.at[0, ph, mid], wbuf.at[0, 0, mid], ws.at[half - 1, 0, mid], wr.at[half - 1, 0, mid],
                            (right * (1 - c) + left * c, z, c)))
    for pos in range(1, m - 1):
        combine_all(0, 1, pos)

    for j in range(1, m):
        for way, t, there in ((0, z - j, z - j >= 0), (1, z + j, z + j < m)):
            for kind, dst in enumerate((dnv, upv)):
                block = dst.at[pl.ds(t * own, own), pl.ds(pl.multiple_of(c * share, 16), share)]
                pl.when(there)(rcopy(
                    block, block, as_.at[way, j - 1, kind], ar.at[way, j - 1, kind], partner).wait_recv)
                start(rcopy(block, block, xs.at[way, j - 1, kind], xr.at[way, j - 1, kind], partner), there)
    for j in range(1, m):
        for way, t, there in ((0, z - j, z - j >= 0), (1, z + j, z + j < m)):
            for kind, dst in enumerate((dnv, upv)):
                block = dst.at[pl.ds(t * own, own), pl.ds(pl.multiple_of((1 - c) * share, 16), share)]
                pl.when(there)(rcopy(
                    block, block, xs.at[way, j - 1, kind], xr.at[way, j - 1, kind], partner).wait_recv)

    @pl.loop(0, blocks)
    def _(b):
        t = tenants_of[b]
        at = pl.ds(pl.multiple_of(b * BLOCK, BLOCK), BLOCK)
        down_t, up_t = dnv[t], upv[t]
        first = nt(tokv[at, :], jnp.concatenate([down_t, jnp.zeros_like(down_t)], axis=0))
        second = nt(cotv[at, :], jnp.concatenate([jnp.zeros_like(up_t), up_t], axis=0))
        sums[z, at, :] = first + second

    for j in range(1, m):
        t = (z + j) % m
        start(rcopy(sums.at[z], sums.at[z], ss.at[j - 1], sr.at[z], plane(t)))

    for i in range(n - 2):
        s = 1 + i + i // (half - 1)
        for q in range(PIECES):
            rcopy(wbuf.at[1, phys(s), q], wbuf.at[1, phys(s), q], ds.at[s, q], dr.at[s, q], partner).wait_recv()

    @pl.loop(0, 2 * (n - 2))
    def _(i):
        k = i // 2
        product(1 + k + k // (half - 1), i % 2, 1 + k)

    for i in range(n - 2):
        s = 1 + i + i // (half - 1)
        forward(((s, 0), (s, 1)), add_hid)
        for pos in range(1, m - 1):
            if i == min(pos - 1, n - 3):
                combine_all(1, n - 2, pos)

    for j in range(1, m):
        t = (z + j) % m
        rcopy(sums.at[t], sums.at[t], ss.at[j - 1], sr.at[t], partner).wait_recv()

    @pl.loop(0, blocks)
    def _(b):
        t = tenants_of[b]
        r = ranks[t]
        at = pl.ds(pl.multiple_of(b * BLOCK, BLOCK), BLOCK)
        total = sums[0, at, :]
        for k in range(1, m):
            total = total + sums[k, at, :]
        lane = lax.broadcasted_iota(jnp.int32, total.shape, 1)
        slot = jnp.where(lane >= rank, lane - rank, lane)
        width = jnp.full(total.shape, r, jnp.int32).astype(F32)
        gain = jnp.where(slot < r, alpha_scale / width, 0.0)
        scaled = (total * gain).astype(BF16)
        column = lax.broadcasted_iota(jnp.int32, (BLOCK, tenants * rank), 1)
        mine = (column >= t * rank) & (column < (t + 1) * rank)
        ada[at, :] = jnp.where(mine, nn(scaled, eye[0]), 0.0).astype(BF16)
        adg[at, :] = jnp.where(mine, nn(scaled, eye[1]), 0.0).astype(BF16)

    tall = gp.shape[0]

    def grads(core, other):
        lanes = pl.ds(pl.multiple_of(core * tall, 128), tall)

        @pl.loop(0, lf // tile)
        def _(j):
            columns = pl.ds(pl.multiple_of(j * tile, tile), tile)
            term = tn(ada[:, lanes], cotv[:, columns])
            if other is not None:
                term = term + other[:, columns].astype(F32)
            gp[:, columns] = term.astype(BF16)

        term = tn(adg[:, lanes], tokv[...])
        if other is not None:
            term = term + other[:, lf:].astype(F32)
        gp[:, lf:] = term.astype(BF16)

    grads(1 - c, None)
    swap = rcopy(gp, dpr, ps.at[0], pr.at[0], partner)
    swap.start()
    swap.wait()
    grads(c, dpr)
    for k in range(1, n):
        peer = snake((place + k) % n, n)
        start(rcopy(gp.at[pl.ds(pl.multiple_of(peer * quarter, 16), quarter)], rsr.at[k - 1], rs.at[k - 1],
                    rr.at[k - 1], (peer, z, c)))

    pl.semaphore_wait(cred.at[2], 1)
    for i in range(mid):
        for way in range(2):
            q = i if way == 0 else PIECES - 1 - i
            arrived(half - 1, way, q, 0)
            across(half, q)
    arrived(half - 1, 0, mid, 0)
    across(half, mid)
    product(half, 0, 0)
    for q in range(PIECES):
        rcopy(wbuf.at[1, 0, q], wbuf.at[1, 0, q], ds.at[half, q], dr.at[half, q], partner).wait_recv()
    product(half, 1, 0)

    for k in range(1, n):
        rcopy(rsr.at[k - 1], rsr.at[k - 1], rs.at[k - 1], rr.at[k - 1], partner).wait_recv()
    total = gp[pl.ds(pl.multiple_of(f * quarter, 16), quarter), :].astype(F32)
    for k in range(1, n):
        total = total + rsr[k - 1].astype(F32)
    ags[...] = total.astype(BF16)
    for k in range(1, n):
        start(rcopy(ags, gr_o.at[f], qs.at[k - 1], qr.at[k - 1], (snake((place + k) % n, n), z, c)))
    keep = pltpu.make_async_copy(ags, gr_o.at[f], o_sem.at[0])
    keep.start()

    for pos in range(1, m - 1):
        for cc in range(2):
            combine(half, cc, pos)

    up_flat = tenants * rank

    def finish(columns, total):
        total = total + nn(ada[...], upv[:, :, columns].reshape(up_flat, tile))
        cotv[:, columns] = (hid[:, columns] + total).astype(BF16)

    forward(((half, 0), (half, 1)), finish)
    hidden = pltpu.make_async_copy(cotv, hid_o, o_sem.at[1])
    hidden.start()

    s_z = (place + n - snake(z, n)) % n
    for slots, cond in (((n,), z == 0), ((s_z,), z == m - 1), ((s_z, n), (z > 0) & (z < m - 1))):
        @pl.when(cond)
        def _():
            for slot in slots:
                for cc in range(2):
                    rcopy(come.at[slot, cc], come.at[slot, cc], gs.at[0, cc], gr.at[slot, cc], partner).wait_recv()
            term = nn(adg[...], dnv[...].reshape(up_flat, ld))
            for ca in range(2):
                cc = ca + c - 2 * ca * c
                total = term[:, ca * depth:(ca + 1) * depth] + part[s_z, cc].astype(F32)
                for slot in slots:
                    total = total + come[slot, cc].astype(F32)
                tokv[:, ca * depth:(ca + 1) * depth] = total.astype(BF16)

    back = pltpu.make_async_copy(tokv, gt_o, o_sem.at[2])
    back.start()

    for k in range(1, n):
        peer = snake((place + n - k) % n, n)
        rcopy(gr_o.at[peer], gr_o.at[peer], qs.at[k - 1], qr.at[k - 1], partner).wait_recv()
    for cond, copy in sent:
        if cond is None:
            copy.wait_send()
        else:
            pl.when(cond)(copy.wait_send)
    for s in range(n):
        for cc in range(2):
            pl.when(owner(s) != z)(hop(s, cc).wait_send)
    keep.wait()
    hidden.wait()
    back.wait()


def make_shards(mesh):
    n, m, dp_n = mesh.shape["fsdp"], mesh.shape["tenant"], mesh.shape["dp"]
    assert dp_n == 2 and n == m and n % 2 == 0 and n >= 4

    def shards(tokens, block_tenant_index, ranks, frozen_up_weight, tenant_down_adapters,
               tenant_up_adapters, cotangent):
        rows, ld = tokens.shape
        lf = cotangent.shape[1]
        tenants = ranks.shape[0]
        rank = tenant_down_adapters.shape[1]
        depth = frozen_up_weight.shape[0]
        piece = depth // PIECES
        tall = tenants * rank // dp_n
        quarter = tall // n
        half = n // 2
        split = tokens
        if depth % 128:
            split = tokens.reshape(rows, ld // depth, depth).transpose(1, 0, 2)
        eye = np.zeros((2, 2 * rank, tenants * rank), np.float32)
        for t in range(tenants):
            for k in range(2):
                eye[k, k * rank:(k + 1) * rank, t * rank:(t + 1) * rank] = np.eye(rank)

        any_space = pl.BlockSpec(memory_space=pl.ANY)
        dma = pltpu.SemaphoreType.DMA
        hidden, back, grads = pl.pallas_call(
            functools.partial(kernel, n, m),
            out_shape=(
                jax.ShapeDtypeStruct((rows, lf), BF16),
                jax.ShapeDtypeStruct((rows, ld), BF16),
                jax.ShapeDtypeStruct((n, quarter, lf + ld), BF16),
            ),
            in_specs=[pl.BlockSpec(memory_space=pltpu.SMEM)] * 2 + [any_space] * 6
            + [pl.BlockSpec(memory_space=pltpu.VMEM)],
            out_specs=(any_space,) * 3,
            scratch_shapes=[
                pltpu.VMEM((2, n - 1, PIECES, piece, lf), BF16),
                pltpu.VMEM((rows, lf), BF16),
                pltpu.VMEM((rows, ld), BF16),
                pltpu.VMEM((m, 2, rows, depth), BF16),
                pltpu.VMEM((rows, lf), F32),
                pltpu.VMEM((tenants, rank, lf), BF16),
                pltpu.VMEM((tenants, rank, ld), BF16),
                pltpu.VMEM((n, 2, rows, depth), BF16),
                pltpu.VMEM((n + 1, 2, rows, depth), BF16),
                pltpu.VMEM((tall, lf + ld), BF16),
                pltpu.VMEM((tall, lf + ld), BF16),
                pltpu.VMEM((n - 1, quarter, lf + ld), BF16),
                pltpu.VMEM((quarter, lf + ld), BF16),
                pltpu.VMEM((m, rows, 2 * rank), F32),
                pltpu.VMEM((rows, tenants * rank), BF16),
                pltpu.VMEM((rows, tenants * rank), BF16),
                dma((7,)),
                dma((half, 2, PIECES)), dma((half, 2, PIECES)),
                dma((1,)), dma((1,)),
                dma((n, PIECES)), dma((n, PIECES)),
                dma((m - 1, 2, 2)), dma((m, 2)),
                dma((2, m - 1, 2)), dma((2, m - 1, 2)),
                dma((2, m - 1, 2)), dma((2, m - 1, 2)),
                dma((m - 1,)), dma((m,)),
                dma((n, 2)), dma((n + 1, 2)),
                dma((1,)), dma((1,)),
                dma((n - 1,)), dma((n - 1,)),
                dma((n - 1,)), dma((n - 1,)),
                dma((3,)),
                pltpu.SemaphoreType.REGULAR((3,)),
            ],
            compiler_params=pltpu.CompilerParams(
                collective_id=0, has_side_effects=True, vmem_limit_bytes=67043328
            ),
        )(block_tenant_index, ranks, tokens, split, cotangent, frozen_up_weight,
          tenant_down_adapters, tenant_up_adapters, jnp.asarray(eye, BF16))
        grads = grads.reshape(tall, lf + ld).astype(F32)
        grad_up = grads[:, :lf].reshape(tenants // dp_n, rank, lf)
        grad_down = grads[:, lf:].reshape(tenants // dp_n, rank, ld)
        return (hidden, back, grad_down, grad_up)

    return shards


def solution(mesh):
    return jax.shard_map(
        make_shards(mesh),
        mesh=mesh,
        in_specs=(
            P(("fsdp", "dp"), "tenant"),
            P(("fsdp", "dp")),
            P(),
            P(("fsdp", "dp"), "tenant"),
            P("tenant", None, None),
            P("tenant", None, None),
            P(("fsdp", "dp"), "tenant"),
        ),
        out_specs=(
            P(("fsdp", "dp"), "tenant"),
            P(("fsdp", "dp"), "tenant"),
            P("dp", None, "tenant"),
            P("dp", None, "tenant"),
        ),
        check_vma=False,
    )
```

```python
import functools
import math

import jax
import jax.numpy as jnp
import numpy as np
from jax import lax
from jax.experimental import pallas as pl
from jax.experimental.pallas import tpu as pltpu
from jax.sharding import PartitionSpec as P

BLOCK = 64
PIECES = 5

alpha_scale = 32.0

BF16 = jnp.bfloat16
F32 = jnp.float32
MESH = pl.DeviceIdType.MESH


def nt(a, b):
    return lax.dot_general(a, b, (((1,), (1,)), ((), ())), preferred_element_type=F32)


def tn(a, b):
    return lax.dot_general(a, b, (((0,), (0,)), ((), ())), preferred_element_type=F32)


def nn(a, b):
    return jnp.dot(a, b, preferred_element_type=F32)


def tile_of(width, most=512):
    return max(t for t in range(128, most + 1, 128) if width % t == 0)


def snake(i, n):
    side = math.isqrt(n)
    if side * side != n:
        return i
    row, col = i // side, i % side
    odd = row % 2
    return row * side + (1 - odd) * col + odd * (side - 1 - col)


def kernel(n, m, tenants_of, ranks, tokens, split, cot, w, dn, up, eye,
           hid_o, gt_o, gu_o, gd_o, pair_o,
           wbuf, cotv, tokv, tv, hid, upv, dnv, part, come, gp, dpr, rsr, ags, sums, ada, adg,
           l_sem, ws, wr, os, orr, ds, dr, ts, tr, as_, ar, xs, xr, ss, sr, gs, gr, ps, pr, rs, rr, qs, qr, o_sem, cred):
    f, z, c = lax.axis_index("fsdp"), lax.axis_index("tenant"), lax.axis_index("dp")
    rows, ld = tokens.shape
    lf = cot.shape[1]
    depth = w.shape[0]
    piece = depth // PIECES
    own, rank, _ = dn.shape
    tenants = ranks.shape[0]
    half = n // 2
    share = rank // 2
    quarter = gp.shape[0] // n
    blocks = rows // BLOCK
    tile = tile_of(lf)
    aligned = depth % 128 == 0

    place = snake(f, n)
    right, left = snake((place + 1) % n, n), snake((place + n - 1) % n, n)
    to_right, to_left, partner = (right, z, c), (left, z, c), (f, z, 1 - c)

    def plane(t):
        return (f, t, c)

    def owner(s):
        return snake((place + n - s) % n, n)

    def phys(s):
        return 0 if s in (0, half) else s if s < half else s - 1

    def rcopy(src, dst, send, recv, device):
        return pltpu.make_async_remote_copy(
            src_ref=src, dst_ref=dst, send_sem=send, recv_sem=recv, device_id=device, device_id_type=MESH
        )

    sent = []

    def start(copy, cond=None):
        if cond is None:
            copy.start()
        else:
            pl.when(cond)(copy.start)
        sent.append((cond, copy))

    barrier = pltpu.get_barrier_semaphore()
    for k in range(1, n):
        pl.semaphore_signal(barrier, inc=1, device_id=(snake((place + k) % n, n), z, c), device_id_type=MESH)
    for k in range(1, m):
        pl.semaphore_signal(barrier, inc=1, device_id=plane((z + k) % m), device_id_type=MESH)
    pl.semaphore_signal(barrier, inc=1, device_id=partner, device_id_type=MESH)

    def tok_src(ca):
        return tokens.at[:, ca * depth:(ca + 1) * depth] if aligned else split.at[ca]

    local = [
        pltpu.make_async_copy(w.reshape(PIECES, piece, lf), wbuf.at[0, 0], l_sem.at[0]),
        pltpu.make_async_copy(cot, cotv, l_sem.at[1]),
        pltpu.make_async_copy(tokens, tokv, l_sem.at[2]),
        pltpu.make_async_copy(tok_src(0), tv.at[z, 0], l_sem.at[3]),
        pltpu.make_async_copy(tok_src(1), tv.at[z, 1], l_sem.at[4]),
        pltpu.make_async_copy(
            dn.at[:, :, pl.ds(pl.multiple_of(z * ld, 128), ld)], dnv.at[pl.ds(z * own, own)], l_sem.at[5]),
        pltpu.make_async_copy(
            up.at[:, :, pl.ds(pl.multiple_of(z * lf, 128), lf)], upv.at[pl.ds(z * own, own)], l_sem.at[6]),
    ]
    for copy in local:
        copy.start()
    pl.semaphore_wait(barrier, n + m - 1)

    pieces = w.reshape(PIECES, piece, lf)
    for i in range(PIECES):
        a, b = i, PIECES - 1 - i
        start(rcopy(pieces.at[a], wbuf.at[0, phys(1), a], ws.at[0, 0, a], wr.at[0, 0, a], to_right))
        start(rcopy(pieces.at[b], wbuf.at[0, phys(n - 1), b], ws.at[0, 1, b], wr.at[0, 1, b], to_left))
    start(rcopy(pieces, wbuf.at[1, 0], os.at[0], orr.at[0], partner))
    start(rcopy(pieces, pair_o, os.at[1], orr.at[1], partner))

    sides = [(way, j, z - j if way == 0 else z + j, (z - j >= 0) if way == 0 else (z + j < m))
             for j in range(1, m) for way in range(2)]
    mine, others = [pl.ds(pl.multiple_of(x * share, 16), share) for x in (c, 1 - c)]
    for j in range(1, m):
        for way, t, there in ((0, z + j, z + j < m), (1, z - j, z - j >= 0)):
            for kind, (src, dst, width) in enumerate(((dn, dnv, ld), (up, upv, lf))):
                start(rcopy(
                    src.at[:, mine, pl.ds(pl.multiple_of(t * width, 128), width)],
                    dst.at[pl.ds(z * own, own), mine],
                    as_.at[way, j - 1, kind], ar.at[way, j - 1, kind], plane(t)), there)
    for ca in range(2):
        start(rcopy(tok_src(ca), tv.at[z, ca], ts.at[0, 0, ca], tr.at[z, ca], plane(z + 1)), z < m - 1)
        start(rcopy(tok_src(ca), tv.at[z, ca], ts.at[0, 1, ca], tr.at[z, ca], plane(z - 1)), z > 0)

    def rows_of(h):
        return pl.ds(pl.multiple_of(h * (rows // 2), 16), rows // 2)

    def hop(s, cc, h):
        d = owner(s)
        upward = (d > z).astype(jnp.int32)
        t = z + 2 * upward - 1
        last_down = (1 - upward) * (t == d).astype(jnp.int32)
        slot = s + (n - s) * last_down
        return rcopy(part.at[s, cc, rows_of(h)], come.at[slot, cc, rows_of(h)], gs.at[s, cc, h], gr.at[slot, cc, h],
                     plane(t))

    def product(s, cc, ph):
        block = wbuf[cc, ph].reshape(depth, lf)
        part[s, cc] = nt(cotv[...], block).astype(BF16)

    def first_hop(s, cc):
        d = owner(s)

        @pl.when(((d > z) & (z == 0)) | ((d < z) & (z == m - 1)))
        def _():
            for h in range(2):
                hop(s, cc, h).start()

    def combine(s, cc, h, pos):
        d = owner(s)
        at = rows_of(h)

        @pl.when(((d > z) & (z == pos)) | ((d < z) & (m - 1 - z == pos)))
        def _():
            rcopy(part.at[s, cc, at], come.at[s, cc, at], gs.at[s, cc, h], gr.at[s, cc, h], partner).wait_recv()
            part[s, cc, at] = (part[s, cc, at].astype(F32) + come[s, cc, at].astype(F32)).astype(BF16)
            hop(s, cc, h).start()

    def combine_all(first, count, pos):
        @pl.loop(0, 4 * count)
        def _(i):
            k = i // 4
            s = first + k + (k // (half - 1)) * (1 if first else 0)
            combine(s, (i // 2) % 2, i % 2, pos)

    local[0].wait()
    local[1].wait()
    product(0, 0, 0)
    rcopy(pieces, wbuf.at[1, 0], os.at[0], orr.at[0], partner).wait_recv()
    product(0, 1, 0)

    pl.semaphore_signal(cred.at[0], inc=1, device_id=to_left, device_id_type=MESH)
    pl.semaphore_signal(cred.at[1], inc=1, device_id=to_right, device_id_type=MESH)
    pl.semaphore_signal(cred.at[2], inc=1, device_id=partner, device_id_type=MESH)
    for copy in local[2:]:
        copy.wait()
    for k in range(3):
        pl.semaphore_wait(cred.at[k], 1)

    mid = PIECES // 2

    def arrived(stage, way, i, ph):
        rcopy(wbuf.at[0, ph, i], wbuf.at[0, ph, i], ws.at[stage, way, i], wr.at[stage, way, i], partner).wait_recv()

    def across(s, i):
        start(rcopy(wbuf.at[0, phys(s), i], wbuf.at[1, phys(s), i], ds.at[s, i], dr.at[s, i], partner))

    def relay(stage, i):
        last = stage == half - 2
        for way in range(2):
            q = i if way == 0 else PIECES - 1 - i
            s = stage + 1 if way == 0 else n - stage - 1
            arrived(stage, way, q, phys(s))
            on = stage + 2 if way == 0 else n - stage - 2
            if not last or i < mid:
                start(rcopy(wbuf.at[0, phys(s), q], wbuf.at[0, phys(on), q], ws.at[stage + 1, way, q],
                            wr.at[stage + 1, way, q], to_right if way == 0 else to_left))
            across(s, q)
        if last and i == mid:
            ph = phys(half - 1) * (1 - c) + phys(half + 1) * c
            start(rcopy(wbuf.at[0, ph, mid], wbuf.at[0, 0, mid], ws.at[half - 1, 0, mid], wr.at[half - 1, 0, mid],
                        (right * (1 - c) + left * c, z, c)))

    for stage in range(half - 2):
        for i in range(PIECES):
            relay(stage, i)
    for i in range(mid):
        relay(half - 2, i)

    for way, j, t, there in sides:
        for kind, dst in enumerate((dnv, upv)):
            block = dst.at[pl.ds(t * own, own), mine]
            pl.when(there)(rcopy(
                block, block, as_.at[way, j - 1, kind], ar.at[way, j - 1, kind], partner).wait_recv)
            start(rcopy(block, block, xs.at[way, j - 1, kind], xr.at[way, j - 1, kind], partner), there)
    for way, j, t, there in sides:
        for kind, dst in enumerate((dnv, upv)):
            block = dst.at[pl.ds(t * own, own), others]
            pl.when(there)(rcopy(
                block, block, xs.at[way, j - 1, kind], xr.at[way, j - 1, kind], partner).wait_recv)

    @pl.loop(0, blocks)
    def _(b):
        t = tenants_of[b]
        at = pl.ds(pl.multiple_of(b * BLOCK, BLOCK), BLOCK)
        down_t, up_t = dnv[t], upv[t]
        first = nt(tokv[at, :], jnp.concatenate([down_t, jnp.zeros_like(down_t)], axis=0))
        second = nt(cotv[at, :], jnp.concatenate([jnp.zeros_like(up_t), up_t], axis=0))
        sums[z, at, :] = first + second

    for j in range(1, m):
        t = (z + j) % m
        start(rcopy(sums.at[z], sums.at[z], ss.at[j - 1], sr.at[z], plane(t)))
    first_hop(0, 0)
    first_hop(0, 1)

    def pass_tokens(k):
        for way, t, there in ((0, z - k, z - k >= 0), (1, z + k, z + k < m)):
            nxt = z + 1 if way == 0 else z - 1
            more = there & ((nxt < m) if way == 0 else (nxt >= 0))
            for ca in range(2):
                pl.when(there)(rcopy(
                    tv.at[t, ca], tv.at[t, ca], ts.at[0, 0, ca], tr.at[t, ca], partner).wait_recv)
                if k < m - 1:
                    start(rcopy(tv.at[t, ca], tv.at[t, ca], ts.at[k, way, ca], tr.at[t, ca], plane(nxt)), more)

    relay(half - 2, mid)
    pass_tokens(1)
    for i in range(mid + 1, PIECES):
        relay(half - 2, i)

    for j in range(1, m):
        t = (z + j) % m
        rcopy(sums.at[t], sums.at[t], ss.at[j - 1], sr.at[t], partner).wait_recv()

    @pl.loop(0, blocks)
    def _(b):
        t = tenants_of[b]
        r = ranks[t]
        at = pl.ds(pl.multiple_of(b * BLOCK, BLOCK), BLOCK)
        total = sums[0, at, :]
        for k in range(1, m):
            total = total + sums[k, at, :]
        lane = lax.broadcasted_iota(jnp.int32, total.shape, 1)
        slot = jnp.where(lane >= rank, lane - rank, lane)
        width = jnp.full(total.shape, r, jnp.int32).astype(F32)
        gain = jnp.where(slot < r, alpha_scale / width, 0.0)
        scaled = (total * gain).astype(BF16)
        column = lax.broadcasted_iota(jnp.int32, (BLOCK, tenants * rank), 1)
        chosen = (column >= t * rank) & (column < (t + 1) * rank)
        ada[at, :] = jnp.where(chosen, nn(scaled, eye[0]), 0.0).astype(BF16)
        adg[at, :] = jnp.where(chosen, nn(scaled, eye[1]), 0.0).astype(BF16)

    tall = gp.shape[0]

    def grads(core, other):
        lanes = pl.ds(pl.multiple_of(core * tall, 128), tall)

        @pl.loop(0, lf // tile)
        def _(j):
            columns = pl.ds(pl.multiple_of(j * tile, tile), tile)
            term = tn(ada[:, lanes], cotv[:, columns])
            if other is not None:
                term = term + other[:, columns].astype(F32)
            gp[:, columns] = term.astype(BF16)

        term = tn(adg[:, lanes], tokv[...])
        if other is not None:
            term = term + other[:, lf:].astype(F32)
        gp[:, lf:] = term.astype(BF16)

    grads(1 - c, None)
    swap = rcopy(gp, dpr, ps.at[0], pr.at[0], partner)
    swap.start()
    combine_all(0, 1, 1)
    swap.wait()
    grads(c, dpr)
    for k in range(2, m - 1):
        pass_tokens(k)

    for i in range(n - 2):
        s = 1 + i + i // (half - 1)
        for q in range(PIECES):
            rcopy(wbuf.at[1, phys(s), q], wbuf.at[1, phys(s), q], ds.at[s, q], dr.at[s, q], partner).wait_recv()

    @pl.loop(0, 2 * (n - 2))
    def _(i):
        k = i // 2
        product(1 + k + k // (half - 1), i % 2, 1 + k)
        first_hop(1 + k + k // (half - 1), i % 2)

    for pos in range(2, m - 1):
        combine_all(0, 1, pos)

    pass_tokens(m - 1)

    def far(i):
        for way in range(2):
            q = i if way == 0 else PIECES - 1 - i
            arrived(half - 1, way, q, 0)
            across(half, q)

    far(0)

    def forward(spots, body):
        spots = [(s, cc, ph if isinstance(ph, tuple) else (cc, ph)) for s, cc, ph in spots]

        @pl.loop(0, lf // tile)
        def _(j):
            columns = pl.ds(pl.multiple_of(j * tile, tile), tile)
            total = None
            for s, cc, ph in spots:
                block = wbuf[ph[0], ph[1], :, :, columns].reshape(depth, tile)
                term = nn(tv[owner(s), c if cc == 0 else 1 - c], block)
                total = term if total is None else total + term
            body(columns, total)

    def set_hid(columns, total):
        hid[:, columns] = total

    def add_hid(columns, total):
        hid[:, columns] += total

    for i in range(n - 2):
        s = 1 + i + i // (half - 1)
        forward(((s, 0, phys(s)), (s, 1, phys(s))), add_hid if i else set_hid)

    for k in range(1, n):
        peer = snake((place + k) % n, n)
        start(rcopy(gp.at[pl.ds(pl.multiple_of(peer * quarter, 16), quarter)], rsr.at[k - 1], rs.at[k - 1],
                    rr.at[k - 1], (peer, z, c)))

    rcopy(pieces, pair_o, os.at[1], orr.at[1], partner).wait_recv()
    again = [pltpu.make_async_copy(pieces, wbuf.at[1, 1], l_sem.at[0]),
             pltpu.make_async_copy(pair_o, wbuf.at[1, 2], l_sem.at[1])]
    for copy in again:
        copy.start()
    for i in range(1, mid):
        far(i)
    combine_all(1, n - 2, 1)
    for copy in again:
        copy.wait()
    forward(((0, 0, (1, 1)), (0, 1, (1, 2))), add_hid)

    arrived(half - 1, 0, mid, 0)
    across(half, mid)
    product(half, 0, 0)
    first_hop(half, 0)
    for q in range(PIECES):
        rcopy(wbuf.at[1, 0, q], wbuf.at[1, 0, q], ds.at[half, q], dr.at[half, q], partner).wait_recv()
    product(half, 1, 0)
    first_hop(half, 1)
    for pos in range(2, m - 1):
        combine_all(1, n - 2, pos)

    up_flat = tenants * rank

    def finish(columns, total):
        total = total + nn(ada[...], upv[:, :, columns].reshape(up_flat, tile))
        cotv[:, columns] = (hid[:, columns] + total).astype(BF16)

    forward(((half, 0, 0), (half, 1, 0)), finish)
    hidden = pltpu.make_async_copy(cotv, hid_o, o_sem.at[2])
    hidden.start()
    for h in range(2):
        combine(half, 0, h, 1)

    for k in range(1, n):
        rcopy(rsr.at[k - 1], rsr.at[k - 1], rs.at[k - 1], rr.at[k - 1], partner).wait_recv()
    total = gp[pl.ds(pl.multiple_of(f * quarter, 16), quarter), :].astype(F32)
    for k in range(1, n):
        total = total + rsr[k - 1].astype(F32)
    ags[...] = total.astype(BF16)
    pair = ((ags.at[:, :lf], gu_o), (ags.at[:, lf:], gd_o))
    keep = [pltpu.make_async_copy(src, dst.at[f], o_sem.at[i]) for i, (src, dst) in enumerate(pair)]
    for k in range(1, n):
        for i, (src, dst) in enumerate(pair):
            start(rcopy(src, dst.at[f], qs.at[k - 1, i], qr.at[k - 1, i], (snake((place + k) % n, n), z, c)))
    for copy in keep:
        copy.start()
    for h in range(2):
        combine(half, 1, h, 1)
    for pos in range(2, m - 1):
        for cc in range(2):
            for h in range(2):
                combine(half, cc, h, pos)

    s_z = (place + n - snake(z, n)) % n
    for slots, cond in (((n,), z == 0), ((s_z,), z == m - 1), ((s_z, n), (z > 0) & (z < m - 1))):
        @pl.when(cond)
        def _():
            for slot in slots:
                for cc in range(2):
                    for h in range(2):
                        at = rows_of(h)
                        rcopy(come.at[slot, cc, at], come.at[slot, cc, at], gs.at[0, cc, h], gr.at[slot, cc, h],
                              partner).wait_recv()
            term = nn(adg[...], dnv[...].reshape(up_flat, ld))
            for ca in range(2):
                cc = ca + c - 2 * ca * c
                total = term[:, ca * depth:(ca + 1) * depth] + part[s_z, cc].astype(F32)
                for slot in slots:
                    total = total + come[slot, cc].astype(F32)
                tokv[:, ca * depth:(ca + 1) * depth] = total.astype(BF16)

    back = pltpu.make_async_copy(tokv, gt_o, o_sem.at[3])
    back.start()

    for k in range(1, n):
        peer = snake((place + n - k) % n, n)
        for i, (_, dst) in enumerate(pair):
            rcopy(dst.at[peer], dst.at[peer], qs.at[k - 1, i], qr.at[k - 1, i], partner).wait_recv()
    for cond, copy in sent:
        if cond is None:
            copy.wait_send()
        else:
            pl.when(cond)(copy.wait_send)
    for s in range(n):
        for cc in range(2):
            for h in range(2):
                pl.when(owner(s) != z)(hop(s, cc, h).wait_send)
    for copy in keep:
        copy.wait()
    hidden.wait()
    back.wait()


def make_shards(mesh):
    n, m, dp_n = mesh.shape["fsdp"], mesh.shape["tenant"], mesh.shape["dp"]
    assert dp_n == 2 and n == m and n % 2 == 0 and n >= 4

    def shards(tokens, block_tenant_index, ranks, frozen_up_weight, tenant_down_adapters,
               tenant_up_adapters, cotangent):
        rows, ld = tokens.shape
        lf = cotangent.shape[1]
        tenants = ranks.shape[0]
        rank = tenant_down_adapters.shape[1]
        depth = frozen_up_weight.shape[0]
        piece = depth // PIECES
        tall = tenants * rank // dp_n
        quarter = tall // n
        half = n // 2
        split = tokens
        if depth % 128:
            split = tokens.reshape(rows, ld // depth, depth).transpose(1, 0, 2)
        eye = np.zeros((2, 2 * rank, tenants * rank), np.float32)
        for t in range(tenants):
            for k in range(2):
                eye[k, k * rank:(k + 1) * rank, t * rank:(t + 1) * rank] = np.eye(rank)

        any_space = pl.BlockSpec(memory_space=pl.ANY)
        dma = pltpu.SemaphoreType.DMA
        hidden, back, grad_up, grad_down, _ = pl.pallas_call(
            functools.partial(kernel, n, m),
            out_shape=(
                jax.ShapeDtypeStruct((rows, lf), BF16),
                jax.ShapeDtypeStruct((rows, ld), BF16),
                jax.ShapeDtypeStruct((n, quarter, lf), BF16),
                jax.ShapeDtypeStruct((n, quarter, ld), BF16),
                jax.ShapeDtypeStruct((PIECES, piece, lf), BF16),
            ),
            in_specs=[pl.BlockSpec(memory_space=pltpu.SMEM)] * 2 + [any_space] * 6
            + [pl.BlockSpec(memory_space=pltpu.VMEM)],
            out_specs=(any_space,) * 5,
            scratch_shapes=[
                pltpu.VMEM((2, n - 1, PIECES, piece, lf), BF16),
                pltpu.VMEM((rows, lf), BF16),
                pltpu.VMEM((rows, ld), BF16),
                pltpu.VMEM((m, 2, rows, depth), BF16),
                pltpu.VMEM((rows, lf), F32),
                pltpu.VMEM((tenants, rank, lf), BF16),
                pltpu.VMEM((tenants, rank, ld), BF16),
                pltpu.VMEM((n, 2, rows, depth), BF16),
                pltpu.VMEM((n + 1, 2, rows, depth), BF16),
                pltpu.VMEM((tall, lf + ld), BF16),
                pltpu.VMEM((tall, lf + ld), BF16),
                pltpu.VMEM((n - 1, quarter, lf + ld), BF16),
                pltpu.VMEM((quarter, lf + ld), BF16),
                pltpu.VMEM((m, rows, 2 * rank), F32),
                pltpu.VMEM((rows, tenants * rank), BF16),
                pltpu.VMEM((rows, tenants * rank), BF16),
                dma((7,)),
                dma((half, 2, PIECES)), dma((half, 2, PIECES)),
                dma((2,)), dma((2,)),
                dma((n, PIECES)), dma((n, PIECES)),
                dma((m - 1, 2, 2)), dma((m, 2)),
                dma((2, m - 1, 2)), dma((2, m - 1, 2)),
                dma((2, m - 1, 2)), dma((2, m - 1, 2)),
                dma((m - 1,)), dma((m,)),
                dma((n, 2, 2)), dma((n + 1, 2, 2)),
                dma((1,)), dma((1,)),
                dma((n - 1,)), dma((n - 1,)),
                dma((n - 1, 2)), dma((n - 1, 2)),
                dma((4,)),
                pltpu.SemaphoreType.REGULAR((3,)),
            ],
            compiler_params=pltpu.CompilerParams(
                collective_id=0, has_side_effects=True, vmem_limit_bytes=67043328
            ),
        )(block_tenant_index, ranks, tokens, split, cotangent, frozen_up_weight,
          tenant_down_adapters, tenant_up_adapters, jnp.asarray(eye, BF16))
        grad_up = grad_up.reshape(tenants // dp_n, rank, lf).astype(F32)
        grad_down = grad_down.reshape(tenants // dp_n, rank, ld).astype(F32)
        return (hidden, back, grad_down, grad_up)

    return shards


def solution(mesh):
    return jax.shard_map(
        make_shards(mesh),
        mesh=mesh,
        in_specs=(
            P(("fsdp", "dp"), "tenant"),
            P(("fsdp", "dp")),
            P(),
            P(("fsdp", "dp"), "tenant"),
            P("tenant", None, None),
            P("tenant", None, None),
            P(("fsdp", "dp"), "tenant"),
        ),
        out_specs=(
            P(("fsdp", "dp"), "tenant"),
            P(("fsdp", "dp"), "tenant"),
            P("dp", None, "tenant"),
            P("dp", None, "tenant"),
        ),
        check_vma=False,
    )
```

```python
import functools
import math

import jax
import jax.numpy as jnp
import numpy as np
from jax import lax
from jax.experimental import pallas as pl
from jax.experimental.pallas import tpu as pltpu
from jax.sharding import PartitionSpec as P

BLOCK = 64
PIECES = 5

alpha_scale = 32.0

BF16 = jnp.bfloat16
F32 = jnp.float32
MESH = pl.DeviceIdType.MESH


def nt(a, b):
    return lax.dot_general(a, b, (((1,), (1,)), ((), ())), preferred_element_type=F32)


def tn(a, b):
    return lax.dot_general(a, b, (((0,), (0,)), ((), ())), preferred_element_type=F32)


def nn(a, b):
    return jnp.dot(a, b, preferred_element_type=F32)


def tile_of(width, most=512):
    return max(t for t in range(128, most + 1, 128) if width % t == 0)


def snake(i, n):
    side = math.isqrt(n)
    if side * side != n:
        return i
    row, col = i // side, i % side
    odd = row % 2
    return row * side + (1 - odd) * col + odd * (side - 1 - col)


def kernel(n, m, tenants_of, ranks, tokens, split, cot, w, dn, up, eye,
           hid_o, gt_o, gu_o, gd_o, pair_o,
           wbuf, cotv, tokv, tv, hid, upv, dnv, part, come, gp, dpr, rsr, ags, sums, ada, adg,
           l_sem, ws, wr, os, orr, ds, dr, ts, tr, as_, ar, xs, xr, ss, sr, gs, gr, ps, pr, rs, rr, qs, qr, o_sem, cred):
    f, z, c = lax.axis_index("fsdp"), lax.axis_index("tenant"), lax.axis_index("dp")
    rows, ld = tokens.shape
    lf = cot.shape[1]
    depth = w.shape[0]
    piece = depth // PIECES
    own, rank, _ = dn.shape
    tenants = ranks.shape[0]
    half = n // 2
    share = rank // 2
    quarter = gp.shape[0] // n
    blocks = rows // BLOCK
    tile = tile_of(lf)
    aligned = depth % 128 == 0

    place = snake(f, n)
    right, left = snake((place + 1) % n, n), snake((place + n - 1) % n, n)
    to_right, to_left, partner = (right, z, c), (left, z, c), (f, z, 1 - c)

    def plane(t):
        return (f, t, c)

    def owner(s):
        return snake((place + n - s) % n, n)

    def phys(s):
        return 0 if s in (0, half) else s if s < half else s - 1

    def rcopy(src, dst, send, recv, device):
        return pltpu.make_async_remote_copy(
            src_ref=src, dst_ref=dst, send_sem=send, recv_sem=recv, device_id=device, device_id_type=MESH
        )

    sent = []

    def start(copy, cond=None):
        if cond is None:
            copy.start()
        else:
            pl.when(cond)(copy.start)
        sent.append((cond, copy))

    barrier = pltpu.get_barrier_semaphore()
    for k in range(1, n):
        pl.semaphore_signal(barrier, inc=1, device_id=(snake((place + k) % n, n), z, c), device_id_type=MESH)
    for k in range(1, m):
        pl.semaphore_signal(barrier, inc=1, device_id=plane((z + k) % m), device_id_type=MESH)
    pl.semaphore_signal(barrier, inc=1, device_id=partner, device_id_type=MESH)

    def tok_src(ca):
        return tokens.at[:, ca * depth:(ca + 1) * depth] if aligned else split.at[ca]

    local = [
        pltpu.make_async_copy(w.reshape(PIECES, piece, lf), wbuf.at[0, 0], l_sem.at[0]),
        pltpu.make_async_copy(cot, cotv, l_sem.at[1]),
        pltpu.make_async_copy(tokens, tokv, l_sem.at[2]),
        pltpu.make_async_copy(tok_src(0), tv.at[z, 0], l_sem.at[3]),
        pltpu.make_async_copy(tok_src(1), tv.at[z, 1], l_sem.at[4]),
        pltpu.make_async_copy(
            dn.at[:, :, pl.ds(pl.multiple_of(z * ld, 128), ld)], dnv.at[pl.ds(z * own, own)], l_sem.at[5]),
        pltpu.make_async_copy(
            up.at[:, :, pl.ds(pl.multiple_of(z * lf, 128), lf)], upv.at[pl.ds(z * own, own)], l_sem.at[6]),
    ]
    for copy in local:
        copy.start()
    pl.semaphore_wait(barrier, n + m - 1)

    pieces = w.reshape(PIECES, piece, lf)
    for i in range(PIECES):
        a, b = i, PIECES - 1 - i
        start(rcopy(pieces.at[a], wbuf.at[0, phys(1), a], ws.at[0, 0, a], wr.at[0, 0, a], to_right))
        start(rcopy(pieces.at[b], wbuf.at[0, phys(n - 1), b], ws.at[0, 1, b], wr.at[0, 1, b], to_left))
    start(rcopy(pieces, wbuf.at[1, 0], os.at[0], orr.at[0], partner))
    start(rcopy(pieces, pair_o, os.at[1], orr.at[1], partner))

    sides = [(way, j, z - j if way == 0 else z + j, (z - j >= 0) if way == 0 else (z + j < m))
             for j in range(1, m) for way in range(2)]
    mine, others = [pl.ds(pl.multiple_of(x * share, 16), share) for x in (c, 1 - c)]
    for j in range(1, m):
        for way, t, there in ((0, z + j, z + j < m), (1, z - j, z - j >= 0)):
            for kind, (src, dst, width) in enumerate(((dn, dnv, ld), (up, upv, lf))):
                start(rcopy(
                    src.at[:, mine, pl.ds(pl.multiple_of(t * width, 128), width)],
                    dst.at[pl.ds(z * own, own), mine],
                    as_.at[way, j - 1, kind], ar.at[way, j - 1, kind], plane(t)), there)
    for ca in range(2):
        start(rcopy(tok_src(ca), tv.at[z, ca], ts.at[0, 0, ca], tr.at[z, ca], plane(z + 1)), z < m - 1)
        start(rcopy(tok_src(ca), tv.at[z, ca], ts.at[0, 1, ca], tr.at[z, ca], plane(z - 1)), z > 0)

    def rows_of(h):
        return pl.ds(pl.multiple_of(h * (rows // 2), 16), rows // 2)

    def hop(s, cc, h):
        d = owner(s)
        upward = (d > z).astype(jnp.int32)
        t = z + 2 * upward - 1
        last_down = (1 - upward) * (t == d).astype(jnp.int32)
        slot = s + (n - s) * last_down
        return rcopy(part.at[s, cc, rows_of(h)], come.at[slot, cc, rows_of(h)], gs.at[s, cc, h], gr.at[slot, cc, h],
                     plane(t))

    def product(s, cc, ph):
        block = wbuf[cc, ph].reshape(depth, lf)
        part[s, cc] = nt(cotv[...], block).astype(BF16)

    def first_hop(s, cc):
        d = owner(s)

        @pl.when(((d > z) & (z == 0)) | ((d < z) & (z == m - 1)))
        def _():
            for h in range(2):
                hop(s, cc, h).start()

    def combine(s, cc, h, pos):
        d = owner(s)
        at = rows_of(h)

        @pl.when(((d > z) & (z == pos)) | ((d < z) & (m - 1 - z == pos)))
        def _():
            rcopy(part.at[s, cc, at], come.at[s, cc, at], gs.at[s, cc, h], gr.at[s, cc, h], partner).wait_recv()
            part[s, cc, at] = (part[s, cc, at].astype(F32) + come[s, cc, at].astype(F32)).astype(BF16)
            hop(s, cc, h).start()

    def combine_own(pos):
        @pl.loop(0, 4)
        def _(i):
            combine(0, i // 2, i % 2, pos)

    def combine_near(cc, pos):
        @pl.loop(0, 2 * (n - 2))
        def _(i):
            k = i // 2
            combine(1 + k + k // (half - 1), cc, i % 2, pos)

    local[0].wait()
    local[1].wait()
    product(0, 0, 0)
    rcopy(pieces, wbuf.at[1, 0], os.at[0], orr.at[0], partner).wait_recv()
    product(0, 1, 0)

    pl.semaphore_signal(cred.at[0], inc=1, device_id=to_left, device_id_type=MESH)
    pl.semaphore_signal(cred.at[1], inc=1, device_id=to_right, device_id_type=MESH)
    pl.semaphore_signal(cred.at[2], inc=1, device_id=partner, device_id_type=MESH)
    for copy in local[2:]:
        copy.wait()
    for k in range(3):
        pl.semaphore_wait(cred.at[k], 1)

    mid = PIECES // 2

    def arrived(stage, way, i, ph):
        rcopy(wbuf.at[0, ph, i], wbuf.at[0, ph, i], ws.at[stage, way, i], wr.at[stage, way, i], partner).wait_recv()

    def across(s, i):
        start(rcopy(wbuf.at[0, phys(s), i], wbuf.at[1, phys(s), i], ds.at[s, i], dr.at[s, i], partner))

    def relay(stage, i):
        last = stage == half - 2
        for way in range(2):
            q = i if way == 0 else PIECES - 1 - i
            s = stage + 1 if way == 0 else n - stage - 1
            arrived(stage, way, q, phys(s))
            on = stage + 2 if way == 0 else n - stage - 2
            if not last or i < mid:
                start(rcopy(wbuf.at[0, phys(s), q], wbuf.at[0, phys(on), q], ws.at[stage + 1, way, q],
                            wr.at[stage + 1, way, q], to_right if way == 0 else to_left))
            across(s, q)
        if last and i == mid:
            ph = phys(half - 1) * (1 - c) + phys(half + 1) * c
            start(rcopy(wbuf.at[0, ph, mid], wbuf.at[0, 0, mid], ws.at[half - 1, 0, mid], wr.at[half - 1, 0, mid],
                        (right * (1 - c) + left * c, z, c)))

    for stage in range(half - 2):
        for i in range(PIECES):
            relay(stage, i)
    for i in range(mid):
        relay(half - 2, i)

    for way, j, t, there in sides:
        for kind, dst in enumerate((dnv, upv)):
            block = dst.at[pl.ds(t * own, own), mine]
            pl.when(there)(rcopy(
                block, block, as_.at[way, j - 1, kind], ar.at[way, j - 1, kind], partner).wait_recv)
            start(rcopy(block, block, xs.at[way, j - 1, kind], xr.at[way, j - 1, kind], partner), there)
    for way, j, t, there in sides:
        for kind, dst in enumerate((dnv, upv)):
            block = dst.at[pl.ds(t * own, own), others]
            pl.when(there)(rcopy(
                block, block, xs.at[way, j - 1, kind], xr.at[way, j - 1, kind], partner).wait_recv)

    @pl.loop(0, blocks)
    def _(b):
        t = tenants_of[b]
        at = pl.ds(pl.multiple_of(b * BLOCK, BLOCK), BLOCK)
        down_t, up_t = dnv[t], upv[t]
        first = nt(tokv[at, :], jnp.concatenate([down_t, jnp.zeros_like(down_t)], axis=0))
        second = nt(cotv[at, :], jnp.concatenate([jnp.zeros_like(up_t), up_t], axis=0))
        sums[z, at, :] = first + second

    for j in range(1, m):
        t = (z + j) % m
        start(rcopy(sums.at[z], sums.at[z], ss.at[j - 1], sr.at[z], plane(t)))
    first_hop(0, 0)
    first_hop(0, 1)

    def pass_tokens(k):
        for way, t, there in ((0, z - k, z - k >= 0), (1, z + k, z + k < m)):
            nxt = z + 1 if way == 0 else z - 1
            more = there & ((nxt < m) if way == 0 else (nxt >= 0))
            for ca in range(2):
                pl.when(there)(rcopy(
                    tv.at[t, ca], tv.at[t, ca], ts.at[0, 0, ca], tr.at[t, ca], partner).wait_recv)
                if k < m - 1:
                    start(rcopy(tv.at[t, ca], tv.at[t, ca], ts.at[k, way, ca], tr.at[t, ca], plane(nxt)), more)

    relay(half - 2, mid)
    pass_tokens(1)
    for i in range(mid + 1, PIECES):
        relay(half - 2, i)

    combine_own(1)
    for i in range(n - 2):
        s = 1 + i + i // (half - 1)
        for q in range(PIECES):
            rcopy(wbuf.at[1, phys(s), q], wbuf.at[1, phys(s), q], ds.at[s, q], dr.at[s, q], partner).wait_recv()

    @pl.loop(0, 2 * (n - 2))
    def _(i):
        k = i % (n - 2)
        product(1 + k + k // (half - 1), i // (n - 2), 1 + k)
        first_hop(1 + k + k // (half - 1), i // (n - 2))

    for j in range(1, m):
        t = (z + j) % m
        rcopy(sums.at[t], sums.at[t], ss.at[j - 1], sr.at[t], partner).wait_recv()

    @pl.loop(0, blocks)
    def _(b):
        t = tenants_of[b]
        r = ranks[t]
        at = pl.ds(pl.multiple_of(b * BLOCK, BLOCK), BLOCK)
        total = sums[0, at, :]
        for k in range(1, m):
            total = total + sums[k, at, :]
        lane = lax.broadcasted_iota(jnp.int32, total.shape, 1)
        slot = jnp.where(lane >= rank, lane - rank, lane)
        width = jnp.full(total.shape, r, jnp.int32).astype(F32)
        gain = jnp.where(slot < r, alpha_scale / width, 0.0)
        scaled = (total * gain).astype(BF16)
        column = lax.broadcasted_iota(jnp.int32, (BLOCK, tenants * rank), 1)
        chosen = (column >= t * rank) & (column < (t + 1) * rank)
        ada[at, :] = jnp.where(chosen, nn(scaled, eye[0]), 0.0).astype(BF16)
        adg[at, :] = jnp.where(chosen, nn(scaled, eye[1]), 0.0).astype(BF16)

    tall = gp.shape[0]

    def grads(core, other):
        lanes = pl.ds(pl.multiple_of(core * tall, 128), tall)

        @pl.loop(0, lf // tile)
        def _(j):
            columns = pl.ds(pl.multiple_of(j * tile, tile), tile)
            term = tn(ada[:, lanes], cotv[:, columns])
            if other is not None:
                term = term + other[:, columns].astype(F32)
            gp[:, columns] = term.astype(BF16)

        term = tn(adg[:, lanes], tokv[...])
        if other is not None:
            term = term + other[:, lf:].astype(F32)
        gp[:, lf:] = term.astype(BF16)

    grads(1 - c, None)
    swap = rcopy(gp, dpr, ps.at[0], pr.at[0], partner)
    swap.start()
    for k in range(2, m - 1):
        pass_tokens(k)
    swap.wait()
    grads(c, dpr)
    for pos in range(2, m - 1):
        combine_own(pos)
    combine_near(0, 1)

    def far(i):
        for way in range(2):
            q = i if way == 0 else PIECES - 1 - i
            arrived(half - 1, way, q, 0)
            across(half, q)

    def forward(spots, body):
        @pl.loop(0, lf // tile)
        def _(j):
            columns = pl.ds(pl.multiple_of(j * tile, tile), tile)
            total = None
            for s, cc, ph in spots:
                block = wbuf[ph[0], ph[1], :, :, columns].reshape(depth, tile)
                term = nn(tv[owner(s), c if cc == 0 else 1 - c], block)
                total = term if total is None else total + term
            body(columns, total)

    def set_hid(columns, total):
        hid[:, columns] = total

    def add_hid(columns, total):
        hid[:, columns] += total

    if n == 4:
        d_first, d_last = owner(1), owner(n - 1)
        later = ((d_first - z) * (d_first - z) > (d_last - z) * (d_last - z)).astype(jnp.int32)
        turns = (later, 1 - later)
    else:
        pass_tokens(m - 1)
        turns = range(n - 2)
    for i, k in enumerate(turns):
        s = 1 + k + k // (half - 1)
        forward(((s, 0, (0, 1 + k)), (s, 1, (1, 1 + k))), add_hid if i else set_hid)
        if n == 4 and i == 0:
            pass_tokens(m - 1)
            far(0)
    if n != 4:
        far(0)

    across_dev = snake((place + half) % n, n)
    hq = quarter // 2
    strip = tile_of(lf + ld)
    merged = n == 4

    def rows_at(dev, h):
        return pl.ds(pl.multiple_of(dev * quarter + h * hq, 16), hq)

    def half_at(h):
        return pl.ds(h * hq, hq)

    def share_to(dev, h, slot, target):
        return rcopy(gp.at[rows_at(dev, h)], rsr.at[slot, half_at(h)], rs.at[slot, h], rr.at[slot, h], target)

    def share_from(slot, h):
        there = rsr.at[slot, half_at(h)]
        rcopy(there, there, rs.at[slot, h], rr.at[slot, h], partner).wait_recv()

    if merged:
        start(share_to(across_dev, 0, 0, to_right))
        start(share_to(across_dev, 1, 0, to_left))
        start(share_to(right, 1, 1, to_right))
        start(share_to(left, 0, 2, to_left))
    else:
        for k in range(1, n):
            peer = snake((place + k) % n, n)
            for h in range(2):
                start(share_to(peer, h, k - 1, (peer, z, c)))

    rcopy(pieces, pair_o, os.at[1], orr.at[1], partner).wait_recv()
    again = [pltpu.make_async_copy(pieces, wbuf.at[1, 1], l_sem.at[0]),
             pltpu.make_async_copy(pair_o, wbuf.at[1, 2], l_sem.at[1])]
    for copy in again:
        copy.start()
    combine_near(1, 1)

    for i in range(1, mid):
        far(i)
    arrived(half - 1, 0, mid, 0)
    across(half, mid)
    product(half, 0, 0)
    first_hop(half, 0)
    for q in range(PIECES):
        rcopy(wbuf.at[1, 0, q], wbuf.at[1, 0, q], ds.at[half, q], dr.at[half, q], partner).wait_recv()
    product(half, 1, 0)
    first_hop(half, 1)
    if merged:
        for h, dev, slot, target in ((0, right, 1, to_right), (1, left, 2, to_left)):
            share_from(0, h)
            at = rows_at(dev, h)

            @pl.loop(0, (lf + ld) // strip)
            def _(j):
                columns = pl.ds(pl.multiple_of(j * strip, strip), strip)
                total = gp[at, columns].astype(F32) + rsr[0, h * hq:(h + 1) * hq, columns].astype(F32)
                gp[at, columns] = total.astype(BF16)

            start(share_to(dev, h, slot, target))
    for pos in range(2, m - 1):
        combine_near(0, pos)
        combine_near(1, pos)

    coming = sorted((2 * cc + h + 1.4 * pos, cc, h, pos) for cc in range(2) for h in range(2) for pos in range(1, m - 1))

    def combine_next(count):
        for _, cc, h, pos in coming[:count]:
            combine(half, cc, h, pos)
        del coming[:count]

    combine_next(1)
    for copy in again:
        copy.wait()
    forward(((0, 0, (1, 1)), (0, 1, (1, 2))), add_hid)
    combine_next(1)

    slots = range(1 if merged else 0, n - 1)
    for slot in slots:
        for h in range(2):
            share_from(slot, h)

    @pl.loop(0, (lf + ld) // strip)
    def _(j):
        columns = pl.ds(pl.multiple_of(j * strip, strip), strip)
        total = gp[pl.ds(pl.multiple_of(f * quarter, 16), quarter), columns].astype(F32)
        for slot in slots:
            total = total + rsr[slot, :, columns].astype(F32)
        ags[:, columns] = total.astype(BF16)

    pair = ((slice(0, lf), gu_o), (slice(lf, lf + ld), gd_o))
    keep = [pltpu.make_async_copy(ags.at[:, lanes], dst.at[f], o_sem.at[i]) for i, (lanes, dst) in enumerate(pair)]

    def result_to(dev, h, slot, target, own_rows):
        for i, (lanes, dst) in enumerate(pair):
            there = dst.at[dev, half_at(h)]
            start(rcopy(ags.at[half_at(h), lanes] if own_rows else there, there, qs.at[slot, h, i], qr.at[slot, h, i],
                        target))

    def result_from(dev, h, slot):
        for i, (_, dst) in enumerate(pair):
            there = dst.at[dev, half_at(h)]
            rcopy(there, there, qs.at[slot, h, i], qr.at[slot, h, i], partner).wait_recv()

    if merged:
        for first in range(2):
            result_to(f, first, 0, to_right, True)
            result_to(f, 1 - first, 1, to_left, True)
    else:
        for k in range(1, n):
            for h in range(2):
                result_to(f, h, k - 1, (snake((place + k) % n, n), z, c), True)
    for copy in keep:
        copy.start()
    combine_next(4)
    if merged:
        result_from(left, 0, 0)
        result_to(left, 0, 2, to_right, False)
        result_from(right, 1, 1)
        result_to(right, 1, 2, to_left, False)
    combine_next(len(coming))

    up_flat = tenants * rank

    def finish(columns, total):
        total = total + nn(ada[...], upv[:, :, columns].reshape(up_flat, tile))
        cotv[:, columns] = (hid[:, columns] + total).astype(BF16)

    forward(((half, 0, (0, 0)), (half, 1, (1, 0))), finish)
    hidden = pltpu.make_async_copy(cotv, hid_o, o_sem.at[2])
    hidden.start()

    s_z = (place + n - snake(z, n)) % n
    for slots, cond in (((n,), z == 0), ((s_z,), z == m - 1), ((s_z, n), (z > 0) & (z < m - 1))):
        @pl.when(cond)
        def _():
            for slot in slots:
                for cc in range(2):
                    for h in range(2):
                        at = rows_of(h)
                        rcopy(come.at[slot, cc, at], come.at[slot, cc, at], gs.at[0, cc, h], gr.at[slot, cc, h],
                              partner).wait_recv()
            term = nn(adg[...], dnv[...].reshape(up_flat, ld))
            for ca in range(2):
                cc = ca + c - 2 * ca * c
                total = term[:, ca * depth:(ca + 1) * depth] + part[s_z, cc].astype(F32)
                for slot in slots:
                    total = total + come[slot, cc].astype(F32)
                tokv[:, ca * depth:(ca + 1) * depth] = total.astype(BF16)

    back = pltpu.make_async_copy(tokv, gt_o, o_sem.at[3])
    back.start()

    if merged:
        for dev, h, slot in ((left, 1, 0), (right, 0, 1), (across_dev, 0, 2), (across_dev, 1, 2)):
            result_from(dev, h, slot)
    else:
        for k in range(1, n):
            for h in range(2):
                result_from(snake((place + n - k) % n, n), h, k - 1)
    for cond, copy in sent:
        if cond is None:
            copy.wait_send()
        else:
            pl.when(cond)(copy.wait_send)
    for s in range(n):
        for cc in range(2):
            for h in range(2):
                pl.when(owner(s) != z)(hop(s, cc, h).wait_send)
    for copy in keep:
        copy.wait()
    hidden.wait()
    back.wait()


def make_shards(mesh):
    n, m, dp_n = mesh.shape["fsdp"], mesh.shape["tenant"], mesh.shape["dp"]
    assert dp_n == 2 and n == m and n % 2 == 0 and n >= 4

    def shards(tokens, block_tenant_index, ranks, frozen_up_weight, tenant_down_adapters,
               tenant_up_adapters, cotangent):
        rows, ld = tokens.shape
        lf = cotangent.shape[1]
        tenants = ranks.shape[0]
        rank = tenant_down_adapters.shape[1]
        depth = frozen_up_weight.shape[0]
        piece = depth // PIECES
        tall = tenants * rank // dp_n
        quarter = tall // n
        half = n // 2
        split = tokens
        if depth % 128:
            split = tokens.reshape(rows, ld // depth, depth).transpose(1, 0, 2)
        eye = np.zeros((2, 2 * rank, tenants * rank), np.float32)
        for t in range(tenants):
            for k in range(2):
                eye[k, k * rank:(k + 1) * rank, t * rank:(t + 1) * rank] = np.eye(rank)

        any_space = pl.BlockSpec(memory_space=pl.ANY)
        dma = pltpu.SemaphoreType.DMA
        hidden, back, grad_up, grad_down, _ = pl.pallas_call(
            functools.partial(kernel, n, m),
            out_shape=(
                jax.ShapeDtypeStruct((rows, lf), BF16),
                jax.ShapeDtypeStruct((rows, ld), BF16),
                jax.ShapeDtypeStruct((n, quarter, lf), BF16),
                jax.ShapeDtypeStruct((n, quarter, ld), BF16),
                jax.ShapeDtypeStruct((PIECES, piece, lf), BF16),
            ),
            in_specs=[pl.BlockSpec(memory_space=pltpu.SMEM)] * 2 + [any_space] * 6
            + [pl.BlockSpec(memory_space=pltpu.VMEM)],
            out_specs=(any_space,) * 5,
            scratch_shapes=[
                pltpu.VMEM((2, n - 1, PIECES, piece, lf), BF16),
                pltpu.VMEM((rows, lf), BF16),
                pltpu.VMEM((rows, ld), BF16),
                pltpu.VMEM((m, 2, rows, depth), BF16),
                pltpu.VMEM((rows, lf), F32),
                pltpu.VMEM((tenants, rank, lf), BF16),
                pltpu.VMEM((tenants, rank, ld), BF16),
                pltpu.VMEM((n, 2, rows, depth), BF16),
                pltpu.VMEM((n + 1, 2, rows, depth), BF16),
                pltpu.VMEM((tall, lf + ld), BF16),
                pltpu.VMEM((tall, lf + ld), BF16),
                pltpu.VMEM((n - 1, quarter, lf + ld), BF16),
                pltpu.VMEM((quarter, lf + ld), BF16),
                pltpu.VMEM((m, rows, 2 * rank), F32),
                pltpu.VMEM((rows, tenants * rank), BF16),
                pltpu.VMEM((rows, tenants * rank), BF16),
                dma((7,)),
                dma((half, 2, PIECES)), dma((half, 2, PIECES)),
                dma((2,)), dma((2,)),
                dma((n, PIECES)), dma((n, PIECES)),
                dma((m - 1, 2, 2)), dma((m, 2)),
                dma((2, m - 1, 2)), dma((2, m - 1, 2)),
                dma((2, m - 1, 2)), dma((2, m - 1, 2)),
                dma((m - 1,)), dma((m,)),
                dma((n, 2, 2)), dma((n + 1, 2, 2)),
                dma((1,)), dma((1,)),
                dma((n - 1, 2)), dma((n - 1, 2)),
                dma((n - 1, 2, 2)), dma((n - 1, 2, 2)),
                dma((4,)),
                pltpu.SemaphoreType.REGULAR((3,)),
            ],
            compiler_params=pltpu.CompilerParams(
                collective_id=0, has_side_effects=True, vmem_limit_bytes=67043328
            ),
        )(block_tenant_index, ranks, tokens, split, cotangent, frozen_up_weight,
          tenant_down_adapters, tenant_up_adapters, jnp.asarray(eye, BF16))
        grad_up = grad_up.reshape(tenants // dp_n, rank, lf).astype(F32)
        grad_down = grad_down.reshape(tenants // dp_n, rank, ld).astype(F32)
        return (hidden, back, grad_down, grad_up)

    return shards


def solution(mesh):
    return jax.shard_map(
        make_shards(mesh),
        mesh=mesh,
        in_specs=(
            P(("fsdp", "dp"), "tenant"),
            P(("fsdp", "dp")),
            P(),
            P(("fsdp", "dp"), "tenant"),
            P("tenant", None, None),
            P("tenant", None, None),
            P(("fsdp", "dp"), "tenant"),
        ),
        out_specs=(
            P(("fsdp", "dp"), "tenant"),
            P(("fsdp", "dp"), "tenant"),
            P("dp", None, "tenant"),
            P("dp", None, "tenant"),
        ),
        check_vma=False,
    )
```

```python
import functools
import math

import jax
import jax.numpy as jnp
import numpy as np
from jax import lax
from jax.experimental import pallas as pl
from jax.experimental.pallas import tpu as pltpu
from jax.sharding import PartitionSpec as P

BLOCK = 64
PIECES = 5

alpha_scale = 32.0

BF16 = jnp.bfloat16
F32 = jnp.float32
MESH = pl.DeviceIdType.MESH


def nt(a, b):
    return lax.dot_general(a, b, (((1,), (1,)), ((), ())), preferred_element_type=F32)


def tn(a, b):
    return lax.dot_general(a, b, (((0,), (0,)), ((), ())), preferred_element_type=F32)


def nn(a, b):
    return jnp.dot(a, b, preferred_element_type=F32)


def tile_of(width, most=512):
    return max(t for t in range(128, most + 1, 128) if width % t == 0)


def snake(i, n):
    side = math.isqrt(n)
    if side * side != n:
        return i
    row, col = i // side, i % side
    odd = row % 2
    return row * side + (1 - odd) * col + odd * (side - 1 - col)


def finish_kernel(hid_i, gt_i, gu_i, gd_i, hid_o, gt_o, gu_o, gd_o, hv, tv, uv, dv, uf, df, i_sem, o_sem):
    n = gu_i.shape[0]
    quarter = gu_i.shape[1]
    fetch = [pltpu.make_async_copy(gu_i.at[k], uv.at[k], i_sem.at[k]) for k in range(n)]
    fetch += [pltpu.make_async_copy(gd_i, dv, i_sem.at[n]), pltpu.make_async_copy(hid_i, hv, i_sem.at[n + 1]),
              pltpu.make_async_copy(gt_i, tv, i_sem.at[n + 2])]
    for copy in fetch:
        copy.start()
    put = []
    for k in range(n):
        fetch[k].wait()
        for r in range(quarter // 16):
            uf[k, r * 16:(r + 1) * 16] = uv[k, r * 16:(r + 1) * 16].astype(F32)
        put.append(pltpu.make_async_copy(uf.at[k], gu_o.at[k], o_sem.at[k]))
        put[-1].start()
    fetch[n].wait()
    for k in range(n):
        df[k] = dv[k].astype(F32)
    put.append(pltpu.make_async_copy(df, gd_o, o_sem.at[n]))
    put[-1].start()
    for i, (src, dst) in enumerate(((hv, hid_o), (tv, gt_o))):
        fetch[n + 1 + i].wait()
        put.append(pltpu.make_async_copy(src, dst, o_sem.at[n + 1 + i]))
        put[-1].start()
    for copy in put:
        copy.wait()


def kernel(n, m, tenants_of, ranks, tokens, split, cot, w, dn, up, eye,
           hid_o, gt_o, gu_o, gd_o, pair_o,
           wbuf, cotv, tokv, tv, hid, upv, dnv, part, come, gp, dpr, rsr, ags, sums, ada, adg,
           l_sem, ws, wr, os, orr, ds, dr, ts, tr, as_, ar, xs, xr, ss, sr, gs, gr, ps, pr, rs, rr, qs, qr, o_sem, cred):
    f, z, c = lax.axis_index("fsdp"), lax.axis_index("tenant"), lax.axis_index("dp")
    rows, ld = tokens.shape
    lf = cot.shape[1]
    depth = w.shape[0]
    piece = depth // PIECES
    own, rank, _ = dn.shape
    tenants = ranks.shape[0]
    half = n // 2
    share = rank // 2
    quarter = gp.shape[0] // n
    blocks = rows // BLOCK
    tile = tile_of(lf)
    aligned = depth % 128 == 0

    place = snake(f, n)
    right, left = snake((place + 1) % n, n), snake((place + n - 1) % n, n)
    to_right, to_left, partner = (right, z, c), (left, z, c), (f, z, 1 - c)

    def plane(t):
        return (f, t, c)

    def owner(s):
        return snake((place + n - s) % n, n)

    def phys(s):
        return 0 if s in (0, half) else s if s < half else s - 1

    def rcopy(src, dst, send, recv, device):
        return pltpu.make_async_remote_copy(
            src_ref=src, dst_ref=dst, send_sem=send, recv_sem=recv, device_id=device, device_id_type=MESH
        )

    sent = []

    def start(copy, cond=None):
        if cond is None:
            copy.start()
        else:
            pl.when(cond)(copy.start)
        sent.append((cond, copy))

    barrier = pltpu.get_barrier_semaphore()
    for k in range(1, n):
        pl.semaphore_signal(barrier, inc=1, device_id=(snake((place + k) % n, n), z, c), device_id_type=MESH)
    for k in range(1, m):
        pl.semaphore_signal(barrier, inc=1, device_id=plane((z + k) % m), device_id_type=MESH)
    pl.semaphore_signal(barrier, inc=1, device_id=partner, device_id_type=MESH)

    def tok_src(ca):
        return tokens.at[:, ca * depth:(ca + 1) * depth] if aligned else split.at[ca]

    local = [
        pltpu.make_async_copy(w.reshape(PIECES, piece, lf), wbuf.at[0, 0], l_sem.at[0]),
        pltpu.make_async_copy(cot, cotv, l_sem.at[1]),
        pltpu.make_async_copy(tokens, tokv, l_sem.at[2]),
        pltpu.make_async_copy(tok_src(0), tv.at[z, 0], l_sem.at[3]),
        pltpu.make_async_copy(tok_src(1), tv.at[z, 1], l_sem.at[4]),
        pltpu.make_async_copy(
            dn.at[:, :, pl.ds(pl.multiple_of(z * ld, 128), ld)], dnv.at[pl.ds(z * own, own)], l_sem.at[5]),
        pltpu.make_async_copy(
            up.at[:, :, pl.ds(pl.multiple_of(z * lf, 128), lf)], upv.at[pl.ds(z * own, own)], l_sem.at[6]),
    ]
    for copy in local:
        copy.start()
    pl.semaphore_wait(barrier, n + m - 1)

    pieces = w.reshape(PIECES, piece, lf)
    for i in range(PIECES):
        a, b = i, PIECES - 1 - i
        start(rcopy(pieces.at[a], wbuf.at[0, phys(1), a], ws.at[0, 0, a], wr.at[0, 0, a], to_right))
        start(rcopy(pieces.at[b], wbuf.at[0, phys(n - 1), b], ws.at[0, 1, b], wr.at[0, 1, b], to_left))
    start(rcopy(pieces, wbuf.at[1, 0], os.at[0], orr.at[0], partner))
    start(rcopy(pieces, pair_o, os.at[1], orr.at[1], partner))

    sides = [(way, j, z - j if way == 0 else z + j, (z - j >= 0) if way == 0 else (z + j < m))
             for j in range(1, m) for way in range(2)]
    mine, others = [pl.ds(pl.multiple_of(x * share, 16), share) for x in (c, 1 - c)]
    for j in range(1, m):
        for way, t, there in ((0, z + j, z + j < m), (1, z - j, z - j >= 0)):
            for kind, (src, dst, width) in enumerate(((dn, dnv, ld), (up, upv, lf))):
                start(rcopy(
                    src.at[:, mine, pl.ds(pl.multiple_of(t * width, 128), width)],
                    dst.at[pl.ds(z * own, own), mine],
                    as_.at[way, j - 1, kind], ar.at[way, j - 1, kind], plane(t)), there)
    for ca in range(2):
        start(rcopy(tok_src(ca), tv.at[z, ca], ts.at[0, 0, ca], tr.at[z, ca], plane(z + 1)), z < m - 1)
        start(rcopy(tok_src(ca), tv.at[z, ca], ts.at[0, 1, ca], tr.at[z, ca], plane(z - 1)), z > 0)

    def rows_of(h):
        return pl.ds(pl.multiple_of(h * (rows // 2), 16), rows // 2)

    def hop(s, cc, h):
        d = owner(s)
        upward = (d > z).astype(jnp.int32)
        t = z + 2 * upward - 1
        last_down = (1 - upward) * (t == d).astype(jnp.int32)
        slot = s + (n - s) * last_down
        return rcopy(part.at[s, cc, rows_of(h)], come.at[slot, cc, rows_of(h)], gs.at[s, cc, h], gr.at[slot, cc, h],
                     plane(t))

    def product(s, cc, ph):
        block = wbuf[cc, ph].reshape(depth, lf)
        part[s, cc] = nt(cotv[...], block).astype(BF16)

    def first_hop(s, cc):
        d = owner(s)

        @pl.when(((d > z) & (z == 0)) | ((d < z) & (z == m - 1)))
        def _():
            for h in range(2):
                hop(s, cc, h).start()

    def combine(s, cc, h, pos):
        d = owner(s)
        at = rows_of(h)

        @pl.when(((d > z) & (z == pos)) | ((d < z) & (m - 1 - z == pos)))
        def _():
            rcopy(part.at[s, cc, at], come.at[s, cc, at], gs.at[s, cc, h], gr.at[s, cc, h], partner).wait_recv()
            part[s, cc, at] = (part[s, cc, at].astype(F32) + come[s, cc, at].astype(F32)).astype(BF16)
            hop(s, cc, h).start()

    def combine_own(pos):
        @pl.loop(0, 4)
        def _(i):
            combine(0, i // 2, i % 2, pos)

    def combine_near(cc, pos):
        @pl.loop(0, 2 * (n - 2))
        def _(i):
            k = i // 2
            combine(1 + k + k // (half - 1), cc, i % 2, pos)

    local[0].wait()
    local[1].wait()
    product(0, 0, 0)
    rcopy(pieces, wbuf.at[1, 0], os.at[0], orr.at[0], partner).wait_recv()
    product(0, 1, 0)

    pl.semaphore_signal(cred.at[0], inc=1, device_id=to_left, device_id_type=MESH)
    pl.semaphore_signal(cred.at[1], inc=1, device_id=to_right, device_id_type=MESH)
    pl.semaphore_signal(cred.at[2], inc=1, device_id=partner, device_id_type=MESH)
    for copy in local[2:]:
        copy.wait()
    for k in range(3):
        pl.semaphore_wait(cred.at[k], 1)

    mid = PIECES // 2

    def arrived(stage, way, i, ph):
        rcopy(wbuf.at[0, ph, i], wbuf.at[0, ph, i], ws.at[stage, way, i], wr.at[stage, way, i], partner).wait_recv()

    def across(s, i):
        start(rcopy(wbuf.at[0, phys(s), i], wbuf.at[1, phys(s), i], ds.at[s, i], dr.at[s, i], partner))

    def relay(stage, i):
        last = stage == half - 2
        for way in range(2):
            q = i if way == 0 else PIECES - 1 - i
            s = stage + 1 if way == 0 else n - stage - 1
            arrived(stage, way, q, phys(s))
            on = stage + 2 if way == 0 else n - stage - 2
            if not last or i < mid:
                start(rcopy(wbuf.at[0, phys(s), q], wbuf.at[0, phys(on), q], ws.at[stage + 1, way, q],
                            wr.at[stage + 1, way, q], to_right if way == 0 else to_left))
            across(s, q)
        if last and i == mid:
            ph = phys(half - 1) * (1 - c) + phys(half + 1) * c
            start(rcopy(wbuf.at[0, ph, mid], wbuf.at[0, 0, mid], ws.at[half - 1, 0, mid], wr.at[half - 1, 0, mid],
                        (right * (1 - c) + left * c, z, c)))

    for stage in range(half - 2):
        for i in range(PIECES):
            relay(stage, i)
    for i in range(mid):
        relay(half - 2, i)

    for way, j, t, there in sides:
        for kind, dst in enumerate((dnv, upv)):
            block = dst.at[pl.ds(t * own, own), mine]
            pl.when(there)(rcopy(
                block, block, as_.at[way, j - 1, kind], ar.at[way, j - 1, kind], partner).wait_recv)
            start(rcopy(block, block, xs.at[way, j - 1, kind], xr.at[way, j - 1, kind], partner), there)
    for way, j, t, there in sides:
        for kind, dst in enumerate((dnv, upv)):
            block = dst.at[pl.ds(t * own, own), others]
            pl.when(there)(rcopy(
                block, block, xs.at[way, j - 1, kind], xr.at[way, j - 1, kind], partner).wait_recv)

    @pl.loop(0, blocks)
    def _(b):
        t = tenants_of[b]
        at = pl.ds(pl.multiple_of(b * BLOCK, BLOCK), BLOCK)
        down_t, up_t = dnv[t], upv[t]
        first = nt(tokv[at, :], jnp.concatenate([down_t, jnp.zeros_like(down_t)], axis=0))
        second = nt(cotv[at, :], jnp.concatenate([jnp.zeros_like(up_t), up_t], axis=0))
        sums[z, at, :] = first + second

    for j in range(1, m):
        t = (z + j) % m
        start(rcopy(sums.at[z], sums.at[z], ss.at[j - 1], sr.at[z], plane(t)))
    first_hop(0, 0)
    first_hop(0, 1)

    def pass_tokens(k):
        for way, t, there in ((0, z - k, z - k >= 0), (1, z + k, z + k < m)):
            nxt = z + 1 if way == 0 else z - 1
            more = there & ((nxt < m) if way == 0 else (nxt >= 0))
            for ca in range(2):
                pl.when(there)(rcopy(
                    tv.at[t, ca], tv.at[t, ca], ts.at[0, 0, ca], tr.at[t, ca], partner).wait_recv)
                if k < m - 1:
                    start(rcopy(tv.at[t, ca], tv.at[t, ca], ts.at[k, way, ca], tr.at[t, ca], plane(nxt)), more)

    relay(half - 2, mid)
    pass_tokens(1)
    for i in range(mid + 1, PIECES):
        relay(half - 2, i)

    combine_own(1)
    for i in range(n - 2):
        s = 1 + i + i // (half - 1)
        for q in range(PIECES):
            rcopy(wbuf.at[1, phys(s), q], wbuf.at[1, phys(s), q], ds.at[s, q], dr.at[s, q], partner).wait_recv()

    @pl.loop(0, 2 * (n - 2))
    def _(i):
        k = i % (n - 2)
        product(1 + k + k // (half - 1), i // (n - 2), 1 + k)
        first_hop(1 + k + k // (half - 1), i // (n - 2))

    for j in range(1, m):
        t = (z + j) % m
        rcopy(sums.at[t], sums.at[t], ss.at[j - 1], sr.at[t], partner).wait_recv()

    @pl.loop(0, blocks)
    def _(b):
        t = tenants_of[b]
        r = ranks[t]
        at = pl.ds(pl.multiple_of(b * BLOCK, BLOCK), BLOCK)
        total = sums[0, at, :]
        for k in range(1, m):
            total = total + sums[k, at, :]
        lane = lax.broadcasted_iota(jnp.int32, total.shape, 1)
        slot = jnp.where(lane >= rank, lane - rank, lane)
        width = jnp.full(total.shape, r, jnp.int32).astype(F32)
        gain = jnp.where(slot < r, alpha_scale / width, 0.0)
        scaled = (total * gain).astype(BF16)
        column = lax.broadcasted_iota(jnp.int32, (BLOCK, tenants * rank), 1)
        chosen = (column >= t * rank) & (column < (t + 1) * rank)
        ada[at, :] = jnp.where(chosen, nn(scaled, eye[0]), 0.0).astype(BF16)
        adg[at, :] = jnp.where(chosen, nn(scaled, eye[1]), 0.0).astype(BF16)

    tall = gp.shape[0]

    def grads(core, other):
        lanes = pl.ds(pl.multiple_of(core * tall, 128), tall)

        @pl.loop(0, lf // tile)
        def _(j):
            columns = pl.ds(pl.multiple_of(j * tile, tile), tile)
            term = tn(ada[:, lanes], cotv[:, columns])
            if other is not None:
                term = term + other[:, columns].astype(F32)
            gp[:, columns] = term.astype(BF16)

        term = tn(adg[:, lanes], tokv[...])
        if other is not None:
            term = term + other[:, lf:].astype(F32)
        gp[:, lf:] = term.astype(BF16)

    grads(1 - c, None)
    swap = rcopy(gp, dpr, ps.at[0], pr.at[0], partner)
    swap.start()
    for k in range(2, m - 1):
        pass_tokens(k)
    swap.wait()
    grads(c, dpr)
    for pos in range(2, m - 1):
        combine_own(pos)
    combine_near(0, 1)

    def far(i):
        for way in range(2):
            q = i if way == 0 else PIECES - 1 - i
            arrived(half - 1, way, q, 0)
            across(half, q)

    def forward(spots, body, first=0, last=lf // tile):
        @pl.loop(first, last)
        def _(j):
            columns = pl.ds(pl.multiple_of(j * tile, tile), tile)
            total = None
            for s, cc, ph in spots:
                block = wbuf[ph[0], ph[1], :, :, columns].reshape(depth, tile)
                term = nn(tv[owner(s), c if cc == 0 else 1 - c], block)
                total = term if total is None else total + term
            body(columns, total)

    def set_hid(columns, total):
        hid[:, columns] = total

    def add_hid(columns, total):
        hid[:, columns] += total

    if n == 4:
        d_first, d_last = owner(1), owner(n - 1)
        later = ((d_first - z) * (d_first - z) > (d_last - z) * (d_last - z)).astype(jnp.int32)
        turns = (later, 1 - later)
    else:
        pass_tokens(m - 1)
        turns = range(n - 2)
    for i, k in enumerate(turns):
        s = 1 + k + k // (half - 1)
        forward(((s, 0, (0, 1 + k)), (s, 1, (1, 1 + k))), add_hid if i else set_hid)
        if n == 4 and i == 0:
            pass_tokens(m - 1)
            far(0)
    if n != 4:
        far(0)

    across_dev = snake((place + half) % n, n)
    hq = quarter // 2
    merged = n == 4

    def rows_at(dev, h):
        return pl.ds(pl.multiple_of(dev * quarter + h * hq, 16), hq)

    def half_at(h):
        return pl.ds(h * hq, hq)

    parts = ((slice(0, lf), gu_o), (slice(lf, lf + ld), gd_o))

    def share_to(i, dev, h, slot, target):
        lanes = parts[i][0]
        return rcopy(gp.at[rows_at(dev, h), lanes], rsr.at[slot, half_at(h), lanes], rs.at[slot, h, i],
                     rr.at[slot, h, i], target)

    def share_from(i, slot, h):
        there = rsr.at[slot, half_at(h), parts[i][0]]
        rcopy(there, there, rs.at[slot, h, i], rr.at[slot, h, i], partner).wait_recv()

    for i in range(2):
        if merged:
            start(share_to(i, across_dev, 0, 0, to_right))
            start(share_to(i, across_dev, 1, 0, to_left))
            start(share_to(i, right, 1, 1, to_right))
            start(share_to(i, left, 0, 2, to_left))
        else:
            for k in range(1, n):
                peer = snake((place + k) % n, n)
                for h in range(2):
                    start(share_to(i, peer, h, k - 1, (peer, z, c)))

    rcopy(pieces, pair_o, os.at[1], orr.at[1], partner).wait_recv()
    again = [pltpu.make_async_copy(pieces, wbuf.at[1, 1], l_sem.at[0]),
             pltpu.make_async_copy(pair_o, wbuf.at[1, 2], l_sem.at[1])]
    for copy in again:
        copy.start()
    combine_near(1, 1)

    for i in range(1, mid):
        far(i)
    arrived(half - 1, 0, mid, 0)
    across(half, mid)
    product(half, 0, 0)
    first_hop(half, 0)
    for q in range(PIECES):
        rcopy(wbuf.at[1, 0, q], wbuf.at[1, 0, q], ds.at[half, q], dr.at[half, q], partner).wait_recv()
    product(half, 1, 0)
    first_hop(half, 1)
    def strips(i, body):
        lanes = parts[i][0]
        strip = tile_of(lanes.stop - lanes.start, 256)

        @pl.loop(0, (lanes.stop - lanes.start) // strip)
        def _(j):
            body(pl.ds(pl.multiple_of(lanes.start + j * strip, 128), strip))

    def merge(i):
        for h, dev, slot, target in ((0, right, 1, to_right), (1, left, 2, to_left)):
            share_from(i, 0, h)
            at = rows_at(dev, h)

            def add(columns):
                total = gp[at, columns].astype(F32) + rsr[0, h * hq:(h + 1) * hq, columns].astype(F32)
                gp[at, columns] = total.astype(BF16)

            strips(i, add)
            start(share_to(i, dev, h, slot, target))

    if merged:
        merge(0)
    for pos in range(2, m - 1):
        combine_near(0, pos)
        combine_near(1, pos)

    coming = sorted((2 * cc + h + 1.4 * pos, cc, h, pos) for cc in range(2) for h in range(2) for pos in range(1, m - 1))

    def combine_next(count):
        for _, cc, h, pos in coming[:count]:
            combine(half, cc, h, pos)
        del coming[:count]

    combine_next(1)
    if merged:
        merge(1)
    for copy in again:
        copy.wait()
    forward(((0, 0, (1, 1)), (0, 1, (1, 2))), add_hid)
    combine_next(1)

    slots = range(1 if merged else 0, n - 1)
    keep = []

    def result_to(i, dev, h, slot, target, own_rows):
        lanes, dst = parts[i]
        there = dst.at[dev, half_at(h)]
        start(rcopy(ags.at[half_at(h), lanes] if own_rows else there, there, qs.at[slot, h, i], qr.at[slot, h, i],
                    target))

    def result_from(i, dev, h, slot):
        there = parts[i][1].at[dev, half_at(h)]
        rcopy(there, there, qs.at[slot, h, i], qr.at[slot, h, i], partner).wait_recv()

    def result(i):
        for slot in slots:
            for h in range(2):
                share_from(i, slot, h)

        def add(columns):
            total = gp[pl.ds(pl.multiple_of(f * quarter, 16), quarter), columns].astype(F32)
            for slot in slots:
                total = total + rsr[slot, :, columns].astype(F32)
            ags[:, columns] = total.astype(BF16)

        strips(i, add)
        if merged:
            for first in range(2):
                result_to(i, f, first, 0, to_right, True)
                result_to(i, f, 1 - first, 1, to_left, True)
        else:
            for k in range(1, n):
                for h in range(2):
                    result_to(i, f, h, k - 1, (snake((place + k) % n, n), z, c), True)
        lanes, dst = parts[i]
        keep.append(pltpu.make_async_copy(ags.at[:, lanes], dst.at[f], o_sem.at[i]))
        keep[-1].start()

    def result_on(i):
        if merged:
            result_from(i, left, 0, 0)
            result_to(i, left, 0, 2, to_right, False)
            result_from(i, right, 1, 1)
            result_to(i, right, 1, 2, to_left, False)

    result(0)
    combine_next(1)
    result(1)
    combine_next(3)
    result_on(0)

    up_flat = tenants * rank
    farthest = ((half, 0, (0, 0)), (half, 1, (1, 0)))
    early = lf // tile // 2

    def finish(columns, total):
        total = total + nn(ada[...], upv[:, :, columns].reshape(up_flat, tile))
        cotv[:, columns] = (hid[:, columns] + total).astype(BF16)

    forward(farthest, finish, 0, early)
    combine_next(len(coming))
    result_on(1)

    forward(farthest, finish, early)
    hidden = pltpu.make_async_copy(cotv, hid_o, o_sem.at[2])
    hidden.start()

    s_z = (place + n - snake(z, n)) % n
    for slots, cond in (((n,), z == 0), ((s_z,), z == m - 1), ((s_z, n), (z > 0) & (z < m - 1))):
        @pl.when(cond)
        def _():
            for slot in slots:
                for cc in range(2):
                    for h in range(2):
                        at = rows_of(h)
                        rcopy(come.at[slot, cc, at], come.at[slot, cc, at], gs.at[0, cc, h], gr.at[slot, cc, h],
                              partner).wait_recv()
            term = nn(adg[...], dnv[...].reshape(up_flat, ld))
            for ca in range(2):
                cc = ca + c - 2 * ca * c
                total = term[:, ca * depth:(ca + 1) * depth] + part[s_z, cc].astype(F32)
                for slot in slots:
                    total = total + come[slot, cc].astype(F32)
                tokv[:, ca * depth:(ca + 1) * depth] = total.astype(BF16)

    back = pltpu.make_async_copy(tokv, gt_o, o_sem.at[3])
    back.start()

    for i in range(2):
        if merged:
            for dev, h, slot in ((left, 1, 0), (right, 0, 1), (across_dev, 0, 2), (across_dev, 1, 2)):
                result_from(i, dev, h, slot)
        else:
            for k in range(1, n):
                for h in range(2):
                    result_from(i, snake((place + n - k) % n, n), h, k - 1)
    for cond, copy in sent:
        if cond is None:
            copy.wait_send()
        else:
            pl.when(cond)(copy.wait_send)
    for s in range(n):
        for cc in range(2):
            for h in range(2):
                pl.when(owner(s) != z)(hop(s, cc, h).wait_send)
    for copy in keep:
        copy.wait()
    hidden.wait()
    back.wait()


def make_shards(mesh):
    n, m, dp_n = mesh.shape["fsdp"], mesh.shape["tenant"], mesh.shape["dp"]
    assert dp_n == 2 and n == m and n % 2 == 0 and n >= 4

    def shards(tokens, block_tenant_index, ranks, frozen_up_weight, tenant_down_adapters,
               tenant_up_adapters, cotangent):
        rows, ld = tokens.shape
        lf = cotangent.shape[1]
        tenants = ranks.shape[0]
        rank = tenant_down_adapters.shape[1]
        depth = frozen_up_weight.shape[0]
        piece = depth // PIECES
        tall = tenants * rank // dp_n
        quarter = tall // n
        half = n // 2
        split = tokens
        if depth % 128:
            split = tokens.reshape(rows, ld // depth, depth).transpose(1, 0, 2)
        eye = np.zeros((2, 2 * rank, tenants * rank), np.float32)
        for t in range(tenants):
            for k in range(2):
                eye[k, k * rank:(k + 1) * rank, t * rank:(t + 1) * rank] = np.eye(rank)

        any_space = pl.BlockSpec(memory_space=pl.ANY)
        dma = pltpu.SemaphoreType.DMA
        hidden, back, grad_up, grad_down, _ = pl.pallas_call(
            functools.partial(kernel, n, m),
            out_shape=(
                jax.ShapeDtypeStruct((rows, lf), BF16),
                jax.ShapeDtypeStruct((rows, ld), BF16),
                jax.ShapeDtypeStruct((n, quarter, lf), BF16),
                jax.ShapeDtypeStruct((n, quarter, ld), BF16),
                jax.ShapeDtypeStruct((PIECES, piece, lf), BF16),
            ),
            in_specs=[pl.BlockSpec(memory_space=pltpu.SMEM)] * 2 + [any_space] * 6
            + [pl.BlockSpec(memory_space=pltpu.VMEM)],
            out_specs=(any_space,) * 5,
            scratch_shapes=[
                pltpu.VMEM((2, n - 1, PIECES, piece, lf), BF16),
                pltpu.VMEM((rows, lf), BF16),
                pltpu.VMEM((rows, ld), BF16),
                pltpu.VMEM((m, 2, rows, depth), BF16),
                pltpu.VMEM((rows, lf), F32),
                pltpu.VMEM((tenants, rank, lf), BF16),
                pltpu.VMEM((tenants, rank, ld), BF16),
                pltpu.VMEM((n, 2, rows, depth), BF16),
                pltpu.VMEM((n + 1, 2, rows, depth), BF16),
                pltpu.VMEM((tall, lf + ld), BF16),
                pltpu.VMEM((tall, lf + ld), BF16),
                pltpu.VMEM((n - 1, quarter, lf + ld), BF16),
                pltpu.VMEM((quarter, lf + ld), BF16),
                pltpu.VMEM((m, rows, 2 * rank), F32),
                pltpu.VMEM((rows, tenants * rank), BF16),
                pltpu.VMEM((rows, tenants * rank), BF16),
                dma((7,)),
                dma((half, 2, PIECES)), dma((half, 2, PIECES)),
                dma((2,)), dma((2,)),
                dma((n, PIECES)), dma((n, PIECES)),
                dma((m - 1, 2, 2)), dma((m, 2)),
                dma((2, m - 1, 2)), dma((2, m - 1, 2)),
                dma((2, m - 1, 2)), dma((2, m - 1, 2)),
                dma((m - 1,)), dma((m,)),
                dma((n, 2, 2)), dma((n + 1, 2, 2)),
                dma((1,)), dma((1,)),
                dma((n - 1, 2, 2)), dma((n - 1, 2, 2)),
                dma((n - 1, 2, 2)), dma((n - 1, 2, 2)),
                dma((4,)),
                pltpu.SemaphoreType.REGULAR((3,)),
            ],
            compiler_params=pltpu.CompilerParams(
                collective_id=0, has_side_effects=True, vmem_limit_bytes=67043328
            ),
        )(block_tenant_index, ranks, tokens, split, cotangent, frozen_up_weight,
          tenant_down_adapters, tenant_up_adapters, jnp.asarray(eye, BF16))
        results = (hidden, back, grad_up, grad_down)
        hidden, back, grad_up, grad_down = pl.pallas_call(
            finish_kernel,
            out_shape=tuple(
                jax.ShapeDtypeStruct(x.shape, F32 if x.ndim == 3 else BF16) for x in results
            ),
            in_specs=[any_space] * 4,
            out_specs=(any_space,) * 4,
            scratch_shapes=[pltpu.VMEM(x.shape, BF16) for x in results]
            + [pltpu.VMEM(x.shape, F32) for x in results[2:]]
            + [dma((n + 3,)), dma((n + 3,))],
            compiler_params=pltpu.CompilerParams(vmem_limit_bytes=67043328),
        )(*results)
        grad_up = grad_up.reshape(tenants // dp_n, rank, lf)
        grad_down = grad_down.reshape(tenants // dp_n, rank, ld)
        return (hidden, back, grad_down, grad_up)

    return shards


def solution(mesh):
    return jax.shard_map(
        make_shards(mesh),
        mesh=mesh,
        in_specs=(
            P(("fsdp", "dp"), "tenant"),
            P(("fsdp", "dp")),
            P(),
            P(("fsdp", "dp"), "tenant"),
            P("tenant", None, None),
            P("tenant", None, None),
            P(("fsdp", "dp"), "tenant"),
        ),
        out_specs=(
            P(("fsdp", "dp"), "tenant"),
            P(("fsdp", "dp"), "tenant"),
            P("dp", None, "tenant"),
            P("dp", None, "tenant"),
        ),
        check_vma=False,
    )
```

```python
import functools
import math

import jax
import jax.numpy as jnp
import numpy as np
from jax import lax
from jax.experimental import pallas as pl
from jax.experimental.pallas import tpu as pltpu
from jax.sharding import PartitionSpec as P

BLOCK = 64
PIECES = 5
BANDS = 4

alpha_scale = 32.0

BF16 = jnp.bfloat16
F32 = jnp.float32
MESH = pl.DeviceIdType.MESH


def nt(a, b):
    return lax.dot_general(a, b, (((1,), (1,)), ((), ())), preferred_element_type=F32)


def tn(a, b):
    return lax.dot_general(a, b, (((0,), (0,)), ((), ())), preferred_element_type=F32)


def nn(a, b):
    return jnp.dot(a, b, preferred_element_type=F32)


def tile_of(width, most=512):
    return max(t for t in range(128, most + 1, 128) if width % t == 0)


def snake(i, n):
    side = math.isqrt(n)
    if side * side != n:
        return i
    row, col = i // side, i % side
    odd = row % 2
    return row * side + (1 - odd) * col + odd * (side - 1 - col)


def finish_kernel(hid_i, gt_i, gu_i, gd_i, hid_o, gt_o, gu_o, gd_o, hv, tv, uv, dv, uf, df, i_sem, o_sem):
    n = gu_i.shape[0]
    quarter = gu_i.shape[1]
    fetch = [pltpu.make_async_copy(gu_i.at[k], uv.at[k], i_sem.at[k]) for k in range(n)]
    fetch += [pltpu.make_async_copy(gd_i, dv, i_sem.at[n]), pltpu.make_async_copy(hid_i, hv, i_sem.at[n + 1]),
              pltpu.make_async_copy(gt_i, tv, i_sem.at[n + 2])]
    for copy in fetch:
        copy.start()
    put = []
    for k in range(n):
        fetch[k].wait()
        for r in range(quarter // 16):
            uf[k, r * 16:(r + 1) * 16] = uv[k, r * 16:(r + 1) * 16].astype(F32)
        put.append(pltpu.make_async_copy(uf.at[k], gu_o.at[k], o_sem.at[k]))
        put[-1].start()
    fetch[n].wait()
    for k in range(n):
        df[k] = dv[k].astype(F32)
    put.append(pltpu.make_async_copy(df, gd_o, o_sem.at[n]))
    put[-1].start()
    for i, (src, dst) in enumerate(((hv, hid_o), (tv, gt_o))):
        fetch[n + 1 + i].wait()
        put.append(pltpu.make_async_copy(src, dst, o_sem.at[n + 1 + i]))
        put[-1].start()
    for copy in put:
        copy.wait()


def kernel(n, m, tenants_of, ranks, tokens, split, cot, w, dn, up, eye,
           hid_o, gt_o, gu_o, gd_o, pair_o,
           wbuf, cotv, tokv, tv, hid, upv, dnv, part, come, gp, dpr, rsr, ags, sums, ada, adg,
           l_sem, ws, wr, os, orr, ds, dr, ts, tr, as_, ar, xs, xr, ss, sr, gs, gr, ps, pr, rs, rr, qs, qr, o_sem, cred):
    f, z, c = lax.axis_index("fsdp"), lax.axis_index("tenant"), lax.axis_index("dp")
    rows, ld = tokens.shape
    lf = cot.shape[1]
    depth = w.shape[0]
    piece = depth // PIECES
    own, rank, _ = dn.shape
    tenants = ranks.shape[0]
    half = n // 2
    share = rank // 2
    quarter = gp.shape[0] // n
    blocks = rows // BLOCK
    tile = tile_of(lf)
    aligned = depth % 128 == 0

    place = snake(f, n)
    right, left = snake((place + 1) % n, n), snake((place + n - 1) % n, n)
    to_right, to_left, partner = (right, z, c), (left, z, c), (f, z, 1 - c)

    def plane(t):
        return (f, t, c)

    def owner(s):
        return snake((place + n - s) % n, n)

    def phys(s):
        return 0 if s in (0, half) else s if s < half else s - 1

    def rcopy(src, dst, send, recv, device):
        return pltpu.make_async_remote_copy(
            src_ref=src, dst_ref=dst, send_sem=send, recv_sem=recv, device_id=device, device_id_type=MESH
        )

    sent = []

    def start(copy, cond=None):
        if cond is None:
            copy.start()
        else:
            pl.when(cond)(copy.start)
        sent.append((cond, copy))

    barrier = pltpu.get_barrier_semaphore()
    for k in range(1, n):
        pl.semaphore_signal(barrier, inc=1, device_id=(snake((place + k) % n, n), z, c), device_id_type=MESH)
    for k in range(1, m):
        pl.semaphore_signal(barrier, inc=1, device_id=plane((z + k) % m), device_id_type=MESH)
    pl.semaphore_signal(barrier, inc=1, device_id=partner, device_id_type=MESH)

    def tok_src(ca):
        return tokens.at[:, ca * depth:(ca + 1) * depth] if aligned else split.at[ca]

    local = [
        pltpu.make_async_copy(w.reshape(PIECES, piece, lf), wbuf.at[0, 0], l_sem.at[0]),
        pltpu.make_async_copy(cot, cotv, l_sem.at[1]),
        pltpu.make_async_copy(tokens, tokv, l_sem.at[2]),
        pltpu.make_async_copy(tok_src(0), tv.at[z, 0], l_sem.at[3]),
        pltpu.make_async_copy(tok_src(1), tv.at[z, 1], l_sem.at[4]),
        pltpu.make_async_copy(
            dn.at[:, :, pl.ds(pl.multiple_of(z * ld, 128), ld)], dnv.at[pl.ds(z * own, own)], l_sem.at[5]),
        pltpu.make_async_copy(
            up.at[:, :, pl.ds(pl.multiple_of(z * lf, 128), lf)], upv.at[pl.ds(z * own, own)], l_sem.at[6]),
    ]
    for copy in local:
        copy.start()
    pl.semaphore_wait(barrier, n + m - 1)

    pieces = w.reshape(PIECES, piece, lf)
    for i in range(PIECES):
        a, b = i, PIECES - 1 - i
        start(rcopy(pieces.at[a], wbuf.at[0, phys(1), a], ws.at[0, 0, a], wr.at[0, 0, a], to_right))
        start(rcopy(pieces.at[b], wbuf.at[0, phys(n - 1), b], ws.at[0, 1, b], wr.at[0, 1, b], to_left))
    start(rcopy(pieces, wbuf.at[1, 0], os.at[0], orr.at[0], partner))
    start(rcopy(pieces, pair_o, os.at[1], orr.at[1], partner))

    sides = [(way, j, z - j if way == 0 else z + j, (z - j >= 0) if way == 0 else (z + j < m))
             for j in range(1, m) for way in range(2)]
    mine, others = [pl.ds(pl.multiple_of(x * share, 16), share) for x in (c, 1 - c)]
    for j in range(1, m):
        for way, t, there in ((0, z + j, z + j < m), (1, z - j, z - j >= 0)):
            for kind, (src, dst, width) in enumerate(((dn, dnv, ld), (up, upv, lf))):
                start(rcopy(
                    src.at[:, mine, pl.ds(pl.multiple_of(t * width, 128), width)],
                    dst.at[pl.ds(z * own, own), mine],
                    as_.at[way, j - 1, kind], ar.at[way, j - 1, kind], plane(t)), there)
    for ca in range(2):
        start(rcopy(tok_src(ca), tv.at[z, ca], ts.at[0, 0, ca], tr.at[z, ca], plane(z + 1)), z < m - 1)
        start(rcopy(tok_src(ca), tv.at[z, ca], ts.at[0, 1, ca], tr.at[z, ca], plane(z - 1)), z > 0)

    def rows_of(h):
        return pl.ds(pl.multiple_of(h * (rows // BANDS), 16), rows // BANDS)

    def hop(s, cc, h):
        d = owner(s)
        upward = (d > z).astype(jnp.int32)
        t = z + 2 * upward - 1
        last_down = (1 - upward) * (t == d).astype(jnp.int32)
        slot = s + (n - s) * last_down
        return rcopy(part.at[s, cc, rows_of(h)], come.at[slot, cc, rows_of(h)], gs.at[s, cc, h], gr.at[slot, cc, h],
                     plane(t))

    def product(s, cc, ph):
        block = wbuf[cc, ph].reshape(depth, lf)
        part[s, cc] = nt(cotv[...], block).astype(BF16)

    def first_hop(s, cc):
        d = owner(s)

        @pl.when(((d > z) & (z == 0)) | ((d < z) & (z == m - 1)))
        def _():
            for h in range(BANDS):
                hop(s, cc, h).start()

    def combine(s, cc, h, pos):
        d = owner(s)
        at = rows_of(h)

        @pl.when(((d > z) & (z == pos)) | ((d < z) & (m - 1 - z == pos)))
        def _():
            rcopy(part.at[s, cc, at], come.at[s, cc, at], gs.at[s, cc, h], gr.at[s, cc, h], partner).wait_recv()
            part[s, cc, at] = (part[s, cc, at].astype(F32) + come[s, cc, at].astype(F32)).astype(BF16)
            hop(s, cc, h).start()

    def combine_own(pos):
        @pl.loop(0, 2 * BANDS)
        def _(i):
            combine(0, i // BANDS, i % BANDS, pos)

    def combine_near(cc, pos):
        @pl.loop(0, BANDS * (n - 2))
        def _(i):
            k = i // BANDS
            combine(1 + k + k // (half - 1), cc, i % BANDS, pos)

    local[0].wait()
    local[1].wait()
    product(0, 0, 0)
    rcopy(pieces, wbuf.at[1, 0], os.at[0], orr.at[0], partner).wait_recv()
    product(0, 1, 0)

    pl.semaphore_signal(cred.at[0], inc=1, device_id=to_left, device_id_type=MESH)
    pl.semaphore_signal(cred.at[1], inc=1, device_id=to_right, device_id_type=MESH)
    pl.semaphore_signal(cred.at[2], inc=1, device_id=partner, device_id_type=MESH)
    for copy in local[2:]:
        copy.wait()
    for k in range(3):
        pl.semaphore_wait(cred.at[k], 1)

    mid = PIECES // 2

    def arrived(stage, way, i, ph):
        rcopy(wbuf.at[0, ph, i], wbuf.at[0, ph, i], ws.at[stage, way, i], wr.at[stage, way, i], partner).wait_recv()

    def across(s, i):
        start(rcopy(wbuf.at[0, phys(s), i], wbuf.at[1, phys(s), i], ds.at[s, i], dr.at[s, i], partner))

    def relay(stage, i):
        last = stage == half - 2
        for way in range(2):
            q = i if way == 0 else PIECES - 1 - i
            s = stage + 1 if way == 0 else n - stage - 1
            arrived(stage, way, q, phys(s))
            on = stage + 2 if way == 0 else n - stage - 2
            if not last or i < mid:
                start(rcopy(wbuf.at[0, phys(s), q], wbuf.at[0, phys(on), q], ws.at[stage + 1, way, q],
                            wr.at[stage + 1, way, q], to_right if way == 0 else to_left))
            across(s, q)
        if last and i == mid:
            ph = phys(half - 1) * (1 - c) + phys(half + 1) * c
            start(rcopy(wbuf.at[0, ph, mid], wbuf.at[0, 0, mid], ws.at[half - 1, 0, mid], wr.at[half - 1, 0, mid],
                        (right * (1 - c) + left * c, z, c)))

    for stage in range(half - 2):
        for i in range(PIECES):
            relay(stage, i)
    for i in range(mid):
        relay(half - 2, i)

    for way, j, t, there in sides:
        for kind, dst in enumerate((dnv, upv)):
            block = dst.at[pl.ds(t * own, own), mine]
            pl.when(there)(rcopy(
                block, block, as_.at[way, j - 1, kind], ar.at[way, j - 1, kind], partner).wait_recv)
            start(rcopy(block, block, xs.at[way, j - 1, kind], xr.at[way, j - 1, kind], partner), there)
    for way, j, t, there in sides:
        for kind, dst in enumerate((dnv, upv)):
            block = dst.at[pl.ds(t * own, own), others]
            pl.when(there)(rcopy(
                block, block, xs.at[way, j - 1, kind], xr.at[way, j - 1, kind], partner).wait_recv)

    @pl.loop(0, blocks)
    def _(b):
        t = tenants_of[b]
        at = pl.ds(pl.multiple_of(b * BLOCK, BLOCK), BLOCK)
        down_t, up_t = dnv[t], upv[t]
        first = nt(tokv[at, :], jnp.concatenate([down_t, jnp.zeros_like(down_t)], axis=0))
        second = nt(cotv[at, :], jnp.concatenate([jnp.zeros_like(up_t), up_t], axis=0))
        sums[z, at, :] = first + second

    for j in range(1, m):
        t = (z + j) % m
        start(rcopy(sums.at[z], sums.at[z], ss.at[j - 1], sr.at[z], plane(t)))
    first_hop(0, 0)
    first_hop(0, 1)

    def pass_tokens(k):
        for way, t, there in ((0, z - k, z - k >= 0), (1, z + k, z + k < m)):
            nxt = z + 1 if way == 0 else z - 1
            more = there & ((nxt < m) if way == 0 else (nxt >= 0))
            for ca in range(2):
                pl.when(there)(rcopy(
                    tv.at[t, ca], tv.at[t, ca], ts.at[0, 0, ca], tr.at[t, ca], partner).wait_recv)
                if k < m - 1:
                    start(rcopy(tv.at[t, ca], tv.at[t, ca], ts.at[k, way, ca], tr.at[t, ca], plane(nxt)), more)

    relay(half - 2, mid)
    pass_tokens(1)
    for i in range(mid + 1, PIECES):
        relay(half - 2, i)

    combine_own(1)
    for i in range(n - 2):
        s = 1 + i + i // (half - 1)
        for q in range(PIECES):
            rcopy(wbuf.at[1, phys(s), q], wbuf.at[1, phys(s), q], ds.at[s, q], dr.at[s, q], partner).wait_recv()

    @pl.loop(0, 2 * (n - 2))
    def _(i):
        k = i % (n - 2)
        product(1 + k + k // (half - 1), i // (n - 2), 1 + k)
        first_hop(1 + k + k // (half - 1), i // (n - 2))

    for j in range(1, m):
        t = (z + j) % m
        rcopy(sums.at[t], sums.at[t], ss.at[j - 1], sr.at[t], partner).wait_recv()

    @pl.loop(0, blocks)
    def _(b):
        t = tenants_of[b]
        r = ranks[t]
        at = pl.ds(pl.multiple_of(b * BLOCK, BLOCK), BLOCK)
        total = sums[0, at, :]
        for k in range(1, m):
            total = total + sums[k, at, :]
        lane = lax.broadcasted_iota(jnp.int32, total.shape, 1)
        slot = jnp.where(lane >= rank, lane - rank, lane)
        width = jnp.full(total.shape, r, jnp.int32).astype(F32)
        gain = jnp.where(slot < r, alpha_scale / width, 0.0)
        scaled = (total * gain).astype(BF16)
        column = lax.broadcasted_iota(jnp.int32, (BLOCK, tenants * rank), 1)
        chosen = (column >= t * rank) & (column < (t + 1) * rank)
        ada[at, :] = jnp.where(chosen, nn(scaled, eye[0]), 0.0).astype(BF16)
        adg[at, :] = jnp.where(chosen, nn(scaled, eye[1]), 0.0).astype(BF16)

    tall = gp.shape[0]

    def grads(core, other):
        lanes = pl.ds(pl.multiple_of(core * tall, 128), tall)

        @pl.loop(0, lf // tile)
        def _(j):
            columns = pl.ds(pl.multiple_of(j * tile, tile), tile)
            term = tn(ada[:, lanes], cotv[:, columns])
            if other is not None:
                term = term + other[:, columns].astype(F32)
            gp[:, columns] = term.astype(BF16)

        term = tn(adg[:, lanes], tokv[...])
        if other is not None:
            term = term + other[:, lf:].astype(F32)
        gp[:, lf:] = term.astype(BF16)

    grads(1 - c, None)
    swap = rcopy(gp, dpr, ps.at[0], pr.at[0], partner)
    swap.start()
    for k in range(2, m - 1):
        pass_tokens(k)
    swap.wait()
    grads(c, dpr)
    for pos in range(2, m - 1):
        combine_own(pos)
    combine_near(0, 1)

    def far(i):
        for way in range(2):
            q = i if way == 0 else PIECES - 1 - i
            arrived(half - 1, way, q, 0)
            across(half, q)

    def forward(spots, body, first=0, last=lf // tile):
        @pl.loop(first, last)
        def _(j):
            columns = pl.ds(pl.multiple_of(j * tile, tile), tile)
            total = None
            for s, cc, ph in spots:
                block = wbuf[ph[0], ph[1], :, :, columns].reshape(depth, tile)
                term = nn(tv[owner(s), c if cc == 0 else 1 - c], block)
                total = term if total is None else total + term
            body(columns, total)

    def set_hid(columns, total):
        hid[:, columns] = total

    def add_hid(columns, total):
        hid[:, columns] += total

    if n == 4:
        d_first, d_last = owner(1), owner(n - 1)
        later = ((d_first - z) * (d_first - z) > (d_last - z) * (d_last - z)).astype(jnp.int32)
        turns = (later, 1 - later)
    else:
        pass_tokens(m - 1)
        turns = range(n - 2)
    for i, k in enumerate(turns):
        s = 1 + k + k // (half - 1)
        forward(((s, 0, (0, 1 + k)), (s, 1, (1, 1 + k))), add_hid if i else set_hid)
        if n == 4 and i == 0:
            pass_tokens(m - 1)
            far(0)
    if n != 4:
        far(0)

    across_dev = snake((place + half) % n, n)
    hq = quarter // 2
    merged = n == 4

    def rows_at(dev, h):
        return pl.ds(pl.multiple_of(dev * quarter + h * hq, 16), hq)

    def half_at(h):
        return pl.ds(h * hq, hq)

    parts = ((slice(0, lf), gu_o), (slice(lf, lf + ld), gd_o))

    def share_to(i, dev, h, slot, target):
        lanes = parts[i][0]
        return rcopy(gp.at[rows_at(dev, h), lanes], rsr.at[slot, half_at(h), lanes], rs.at[slot, h, i],
                     rr.at[slot, h, i], target)

    def share_from(i, slot, h):
        there = rsr.at[slot, half_at(h), parts[i][0]]
        rcopy(there, there, rs.at[slot, h, i], rr.at[slot, h, i], partner).wait_recv()

    for i in range(2):
        if merged:
            start(share_to(i, across_dev, 0, 0, to_right))
            start(share_to(i, across_dev, 1, 0, to_left))
            start(share_to(i, right, 1, 1, to_right))
            start(share_to(i, left, 0, 2, to_left))
        else:
            for k in range(1, n):
                peer = snake((place + k) % n, n)
                for h in range(2):
                    start(share_to(i, peer, h, k - 1, (peer, z, c)))

    rcopy(pieces, pair_o, os.at[1], orr.at[1], partner).wait_recv()
    again = [pltpu.make_async_copy(pieces, wbuf.at[1, 1], l_sem.at[0]),
             pltpu.make_async_copy(pair_o, wbuf.at[1, 2], l_sem.at[1])]
    for copy in again:
        copy.start()
    combine_near(1, 1)

    for i in range(1, mid):
        far(i)
    arrived(half - 1, 0, mid, 0)
    across(half, mid)
    product(half, 0, 0)
    first_hop(half, 0)
    for q in range(PIECES):
        rcopy(wbuf.at[1, 0, q], wbuf.at[1, 0, q], ds.at[half, q], dr.at[half, q], partner).wait_recv()
    product(half, 1, 0)
    first_hop(half, 1)
    def strips(i, body):
        lanes = parts[i][0]
        strip = tile_of(lanes.stop - lanes.start, 256)

        @pl.loop(0, (lanes.stop - lanes.start) // strip)
        def _(j):
            body(pl.ds(pl.multiple_of(lanes.start + j * strip, 128), strip))

    def merge(i):
        for h, dev, slot, target in ((0, right, 1, to_right), (1, left, 2, to_left)):
            share_from(i, 0, h)
            at = rows_at(dev, h)

            def add(columns):
                total = gp[at, columns].astype(F32) + rsr[0, h * hq:(h + 1) * hq, columns].astype(F32)
                gp[at, columns] = total.astype(BF16)

            strips(i, add)
            start(share_to(i, dev, h, slot, target))

    if merged:
        merge(0)
    for pos in range(2, m - 1):
        combine_near(0, pos)
        combine_near(1, pos)

    coming = sorted(
        (BANDS * cc + h + 2 * pos, pos, cc, h) for cc in range(2) for h in range(BANDS) for pos in range(1, m - 1))

    def combine_next(count):
        for _, pos, cc, h in coming[:count]:
            combine(half, cc, h, pos)
        del coming[:count]

    combine_next(2)
    if merged:
        merge(1)
    for copy in again:
        copy.wait()
    forward(((0, 0, (1, 1)), (0, 1, (1, 2))), add_hid)
    combine_next(4)

    slots = range(1 if merged else 0, n - 1)
    keep = []

    def result_to(i, dev, h, slot, target, own_rows):
        lanes, dst = parts[i]
        there = dst.at[dev, half_at(h)]
        start(rcopy(ags.at[half_at(h), lanes] if own_rows else there, there, qs.at[slot, h, i], qr.at[slot, h, i],
                    target))

    def result_from(i, dev, h, slot):
        there = parts[i][1].at[dev, half_at(h)]
        rcopy(there, there, qs.at[slot, h, i], qr.at[slot, h, i], partner).wait_recv()

    def result(i):
        for slot in slots:
            for h in range(2):
                share_from(i, slot, h)

        def add(columns):
            total = gp[pl.ds(pl.multiple_of(f * quarter, 16), quarter), columns].astype(F32)
            for slot in slots:
                total = total + rsr[slot, :, columns].astype(F32)
            ags[:, columns] = total.astype(BF16)

        strips(i, add)
        if merged:
            for first in range(2):
                result_to(i, f, first, 0, to_right, True)
                result_to(i, f, 1 - first, 1, to_left, True)
        else:
            for k in range(1, n):
                for h in range(2):
                    result_to(i, f, h, k - 1, (snake((place + k) % n, n), z, c), True)
        lanes, dst = parts[i]
        keep.append(pltpu.make_async_copy(ags.at[:, lanes], dst.at[f], o_sem.at[i]))
        keep[-1].start()

    def result_on(i):
        if merged:
            result_from(i, left, 0, 0)
            result_to(i, left, 0, 2, to_right, False)
            result_from(i, right, 1, 1)
            result_to(i, right, 1, 2, to_left, False)

    result(0)
    result(1)
    combine_next(6)
    result_on(0)

    up_flat = tenants * rank
    farthest = ((half, 0, (0, 0)), (half, 1, (1, 0)))
    early = lf // tile // 2

    def finish(columns, total):
        total = total + nn(ada[...], upv[:, :, columns].reshape(up_flat, tile))
        cotv[:, columns] = (hid[:, columns] + total).astype(BF16)

    combine_next(2)
    forward(farthest, finish, 0, early)
    combine_next(len(coming))
    result_on(1)

    forward(farthest, finish, early)
    hidden = pltpu.make_async_copy(cotv, hid_o, o_sem.at[2])
    hidden.start()

    s_z = (place + n - snake(z, n)) % n
    for slots, cond in (((n,), z == 0), ((s_z,), z == m - 1), ((s_z, n), (z > 0) & (z < m - 1))):
        @pl.when(cond)
        def _():
            for slot in slots:
                for cc in range(2):
                    for h in range(BANDS):
                        at = rows_of(h)
                        rcopy(come.at[slot, cc, at], come.at[slot, cc, at], gs.at[0, cc, h], gr.at[slot, cc, h],
                              partner).wait_recv()
            term = nn(adg[...], dnv[...].reshape(up_flat, ld))
            for ca in range(2):
                cc = ca + c - 2 * ca * c
                total = term[:, ca * depth:(ca + 1) * depth] + part[s_z, cc].astype(F32)
                for slot in slots:
                    total = total + come[slot, cc].astype(F32)
                tokv[:, ca * depth:(ca + 1) * depth] = total.astype(BF16)

    back = pltpu.make_async_copy(tokv, gt_o, o_sem.at[3])
    back.start()

    for i in range(2):
        if merged:
            for dev, h, slot in ((left, 1, 0), (right, 0, 1), (across_dev, 0, 2), (across_dev, 1, 2)):
                result_from(i, dev, h, slot)
        else:
            for k in range(1, n):
                for h in range(2):
                    result_from(i, snake((place + n - k) % n, n), h, k - 1)
    for cond, copy in sent:
        if cond is None:
            copy.wait_send()
        else:
            pl.when(cond)(copy.wait_send)
    for s in range(n):
        for cc in range(2):
            for h in range(BANDS):
                pl.when(owner(s) != z)(hop(s, cc, h).wait_send)
    for copy in keep:
        copy.wait()
    hidden.wait()
    back.wait()


def make_shards(mesh):
    n, m, dp_n = mesh.shape["fsdp"], mesh.shape["tenant"], mesh.shape["dp"]
    assert dp_n == 2 and n == m and n % 2 == 0 and n >= 4

    def shards(tokens, block_tenant_index, ranks, frozen_up_weight, tenant_down_adapters,
               tenant_up_adapters, cotangent):
        rows, ld = tokens.shape
        lf = cotangent.shape[1]
        tenants = ranks.shape[0]
        rank = tenant_down_adapters.shape[1]
        depth = frozen_up_weight.shape[0]
        piece = depth // PIECES
        tall = tenants * rank // dp_n
        quarter = tall // n
        half = n // 2
        split = tokens
        if depth % 128:
            split = tokens.reshape(rows, ld // depth, depth).transpose(1, 0, 2)
        eye = np.zeros((2, 2 * rank, tenants * rank), np.float32)
        for t in range(tenants):
            for k in range(2):
                eye[k, k * rank:(k + 1) * rank, t * rank:(t + 1) * rank] = np.eye(rank)

        any_space = pl.BlockSpec(memory_space=pl.ANY)
        dma = pltpu.SemaphoreType.DMA
        hidden, back, grad_up, grad_down, _ = pl.pallas_call(
            functools.partial(kernel, n, m),
            out_shape=(
                jax.ShapeDtypeStruct((rows, lf), BF16),
                jax.ShapeDtypeStruct((rows, ld), BF16),
                jax.ShapeDtypeStruct((n, quarter, lf), BF16),
                jax.ShapeDtypeStruct((n, quarter, ld), BF16),
                jax.ShapeDtypeStruct((PIECES, piece, lf), BF16),
            ),
            in_specs=[pl.BlockSpec(memory_space=pltpu.SMEM)] * 2 + [any_space] * 6
            + [pl.BlockSpec(memory_space=pltpu.VMEM)],
            out_specs=(any_space,) * 5,
            scratch_shapes=[
                pltpu.VMEM((2, n - 1, PIECES, piece, lf), BF16),
                pltpu.VMEM((rows, lf), BF16),
                pltpu.VMEM((rows, ld), BF16),
                pltpu.VMEM((m, 2, rows, depth), BF16),
                pltpu.VMEM((rows, lf), F32),
                pltpu.VMEM((tenants, rank, lf), BF16),
                pltpu.VMEM((tenants, rank, ld), BF16),
                pltpu.VMEM((n, 2, rows, depth), BF16),
                pltpu.VMEM((n + 1, 2, rows, depth), BF16),
                pltpu.VMEM((tall, lf + ld), BF16),
                pltpu.VMEM((tall, lf + ld), BF16),
                pltpu.VMEM((n - 1, quarter, lf + ld), BF16),
                pltpu.VMEM((quarter, lf + ld), BF16),
                pltpu.VMEM((m, rows, 2 * rank), F32),
                pltpu.VMEM((rows, tenants * rank), BF16),
                pltpu.VMEM((rows, tenants * rank), BF16),
                dma((7,)),
                dma((half, 2, PIECES)), dma((half, 2, PIECES)),
                dma((2,)), dma((2,)),
                dma((n, PIECES)), dma((n, PIECES)),
                dma((m - 1, 2, 2)), dma((m, 2)),
                dma((2, m - 1, 2)), dma((2, m - 1, 2)),
                dma((2, m - 1, 2)), dma((2, m - 1, 2)),
                dma((m - 1,)), dma((m,)),
                dma((n, 2, BANDS)), dma((n + 1, 2, BANDS)),
                dma((1,)), dma((1,)),
                dma((n - 1, 2, 2)), dma((n - 1, 2, 2)),
                dma((n - 1, 2, 2)), dma((n - 1, 2, 2)),
                dma((4,)),
                pltpu.SemaphoreType.REGULAR((3,)),
            ],
            compiler_params=pltpu.CompilerParams(
                collective_id=0, has_side_effects=True, vmem_limit_bytes=67043328
            ),
        )(block_tenant_index, ranks, tokens, split, cotangent, frozen_up_weight,
          tenant_down_adapters, tenant_up_adapters, jnp.asarray(eye, BF16))
        results = (hidden, back, grad_up, grad_down)
        hidden, back, grad_up, grad_down = pl.pallas_call(
            finish_kernel,
            out_shape=tuple(
                jax.ShapeDtypeStruct(x.shape, F32 if x.ndim == 3 else BF16) for x in results
            ),
            in_specs=[any_space] * 4,
            out_specs=(any_space,) * 4,
            scratch_shapes=[pltpu.VMEM(x.shape, BF16) for x in results]
            + [pltpu.VMEM(x.shape, F32) for x in results[2:]]
            + [dma((n + 3,)), dma((n + 3,))],
            compiler_params=pltpu.CompilerParams(vmem_limit_bytes=67043328),
        )(*results)
        grad_up = grad_up.reshape(tenants // dp_n, rank, lf)
        grad_down = grad_down.reshape(tenants // dp_n, rank, ld)
        return (hidden, back, grad_down, grad_up)

    return shards


def solution(mesh):
    return jax.shard_map(
        make_shards(mesh),
        mesh=mesh,
        in_specs=(
            P(("fsdp", "dp"), "tenant"),
            P(("fsdp", "dp")),
            P(),
            P(("fsdp", "dp"), "tenant"),
            P("tenant", None, None),
            P("tenant", None, None),
            P(("fsdp", "dp"), "tenant"),
        ),
        out_specs=(
            P(("fsdp", "dp"), "tenant"),
            P(("fsdp", "dp"), "tenant"),
            P("dp", None, "tenant"),
            P("dp", None, "tenant"),
        ),
        check_vma=False,
    )
```

```python
import functools
import math

import jax
import jax.numpy as jnp
import numpy as np
from jax import lax
from jax.experimental import pallas as pl
from jax.experimental.pallas import tpu as pltpu
from jax.sharding import PartitionSpec as P

BLOCK = 64
PIECES = 5
BANDS = 4

alpha_scale = 32.0

BF16 = jnp.bfloat16
F32 = jnp.float32
MESH = pl.DeviceIdType.MESH


def nt(a, b):
    return lax.dot_general(a, b, (((1,), (1,)), ((), ())), preferred_element_type=F32)


def tn(a, b):
    return lax.dot_general(a, b, (((0,), (0,)), ((), ())), preferred_element_type=F32)


def nn(a, b):
    return jnp.dot(a, b, preferred_element_type=F32)


def tile_of(width, most=512):
    return max(t for t in range(128, most + 1, 128) if width % t == 0)


def snake(i, n):
    side = math.isqrt(n)
    if side * side != n:
        return i
    row, col = i // side, i % side
    odd = row % 2
    return row * side + (1 - odd) * col + odd * (side - 1 - col)


def finish_kernel(hid_i, gt_i, gu_i, gd_i, hid_o, gt_o, gu_o, gd_o, hv, tv, uv, dv, uf, df, i_sem, o_sem):
    n = gu_i.shape[0]
    quarter = gu_i.shape[1]
    plain = [pltpu.make_async_copy(hid_i, hv, i_sem.at[n + 1]), pltpu.make_async_copy(gt_i, tv, i_sem.at[n + 2])]
    fetch = [pltpu.make_async_copy(gu_i.at[k], uv.at[k], i_sem.at[k]) for k in range(n)]
    fetch.append(pltpu.make_async_copy(gd_i, dv, i_sem.at[n]))
    for copy in fetch[:1] + plain[:1] + fetch[1:] + plain[1:]:
        copy.start()
    put = []

    def out(src, dst, k):
        put.append(pltpu.make_async_copy(src, dst, o_sem.at[k]))
        put[-1].start()

    for k in range(n):
        fetch[k].wait()
        for r in range(quarter // 16):
            uf[k, r * 16:(r + 1) * 16] = uv[k, r * 16:(r + 1) * 16].astype(F32)
        out(uf.at[k], gu_o.at[k], k)
        if k == 0:
            plain[0].wait()
            out(hv, hid_o, n + 1)
    fetch[n].wait()
    for k in range(n):
        df[k] = dv[k].astype(F32)
    out(df, gd_o, n)
    plain[1].wait()
    out(tv, gt_o, n + 2)
    for copy in put:
        copy.wait()


def kernel(n, m, tenants_of, ranks, tokens, split, cot, w, dn, up, eye_i,
           hid_o, gt_o, gu_o, gd_o, pair_o,
           wbuf, cotv, tokv, tv, hid, upv, dnv, part, come, gp, dpr, rsr, ags, sums, ada, adg, eye,
           l_sem, ws, wr, os, orr, ds, dr, ts, tr, as_, ar, xs, xr, ss, sr, gs, gr, ps, pr, rs, rr, qs, qr, o_sem, cred):
    f, z, c = lax.axis_index("fsdp"), lax.axis_index("tenant"), lax.axis_index("dp")
    rows, ld = tokens.shape
    lf = cot.shape[1]
    depth = w.shape[0]
    piece = depth // PIECES
    own, rank, _ = dn.shape
    tenants = ranks.shape[0]
    half = n // 2
    share = rank // 2
    quarter = gp.shape[0] // n
    blocks = rows // BLOCK
    tile = tile_of(lf)
    aligned = depth % 128 == 0

    place = snake(f, n)
    right, left = snake((place + 1) % n, n), snake((place + n - 1) % n, n)
    to_right, to_left, partner = (right, z, c), (left, z, c), (f, z, 1 - c)

    def plane(t):
        return (f, t, c)

    def owner(s):
        return snake((place + n - s) % n, n)

    def phys(s):
        return 0 if s in (0, half) else s if s < half else s - 1

    def rcopy(src, dst, send, recv, device):
        return pltpu.make_async_remote_copy(
            src_ref=src, dst_ref=dst, send_sem=send, recv_sem=recv, device_id=device, device_id_type=MESH
        )

    sent = []

    def start(copy, cond=None):
        if cond is None:
            copy.start()
        else:
            pl.when(cond)(copy.start)
        sent.append((cond, copy))

    barrier = pltpu.get_barrier_semaphore()
    for k in range(1, n):
        pl.semaphore_signal(barrier, inc=1, device_id=(snake((place + k) % n, n), z, c), device_id_type=MESH)
    for k in range(1, m):
        pl.semaphore_signal(barrier, inc=1, device_id=plane((z + k) % m), device_id_type=MESH)
    pl.semaphore_signal(barrier, inc=1, device_id=partner, device_id_type=MESH)

    def tok_src(ca):
        return tokens.at[:, ca * depth:(ca + 1) * depth] if aligned else split.at[ca]

    local = [
        pltpu.make_async_copy(w.reshape(PIECES, piece, lf), wbuf.at[0, 0], l_sem.at[0]),
        pltpu.make_async_copy(cot, cotv, l_sem.at[1]),
        pltpu.make_async_copy(tokens, tokv, l_sem.at[2]),
        pltpu.make_async_copy(tok_src(0), tv.at[z, 0], l_sem.at[3]),
        pltpu.make_async_copy(tok_src(1), tv.at[z, 1], l_sem.at[4]),
        pltpu.make_async_copy(
            dn.at[:, :, pl.ds(pl.multiple_of(z * ld, 128), ld)], dnv.at[pl.ds(z * own, own)], l_sem.at[5]),
        pltpu.make_async_copy(
            up.at[:, :, pl.ds(pl.multiple_of(z * lf, 128), lf)], upv.at[pl.ds(z * own, own)], l_sem.at[6]),
        pltpu.make_async_copy(eye_i, eye, l_sem.at[7]),
    ]
    for copy in local:
        copy.start()
    pl.semaphore_wait(barrier, n + m - 1)

    pieces = w.reshape(PIECES, piece, lf)
    for i in range(PIECES):
        a, b = i, PIECES - 1 - i
        start(rcopy(pieces.at[a], wbuf.at[0, phys(1), a], ws.at[0, 0, a], wr.at[0, 0, a], to_right))
        start(rcopy(pieces.at[b], wbuf.at[0, phys(n - 1), b], ws.at[0, 1, b], wr.at[0, 1, b], to_left))
    start(rcopy(pieces, wbuf.at[1, 0], os.at[0], orr.at[0], partner))
    start(rcopy(pieces, pair_o, os.at[1], orr.at[1], partner))

    sides = [(way, j, z - j if way == 0 else z + j, (z - j >= 0) if way == 0 else (z + j < m))
             for j in range(1, m) for way in range(2)]
    mine, others = [pl.ds(pl.multiple_of(x * share, 16), share) for x in (c, 1 - c)]
    for j in range(1, m):
        for way, t, there in ((0, z + j, z + j < m), (1, z - j, z - j >= 0)):
            for kind, (src, dst, width) in enumerate(((dn, dnv, ld), (up, upv, lf))):
                start(rcopy(
                    src.at[:, mine, pl.ds(pl.multiple_of(t * width, 128), width)],
                    dst.at[pl.ds(z * own, own), mine],
                    as_.at[way, j - 1, kind], ar.at[way, j - 1, kind], plane(t)), there)
    for ca in range(2):
        start(rcopy(tok_src(ca), tv.at[z, ca], ts.at[0, 0, ca], tr.at[z, ca], plane(z + 1)), z < m - 1)
        start(rcopy(tok_src(ca), tv.at[z, ca], ts.at[0, 1, ca], tr.at[z, ca], plane(z - 1)), z > 0)

    def rows_of(h):
        return pl.ds(pl.multiple_of(h * (rows // BANDS), 16), rows // BANDS)

    def hop(s, cc, h):
        d = owner(s)
        upward = (d > z).astype(jnp.int32)
        t = z + 2 * upward - 1
        last_down = (1 - upward) * (t == d).astype(jnp.int32)
        slot = s + (n - s) * last_down
        return rcopy(part.at[s, cc, rows_of(h)], come.at[slot, cc, rows_of(h)], gs.at[s, cc, h], gr.at[slot, cc, h],
                     plane(t))

    def product(s, cc, ph):
        block = wbuf[cc, ph].reshape(depth, lf)
        part[s, cc] = nt(cotv[...], block).astype(BF16)

    def first_hop(s, cc):
        d = owner(s)

        @pl.when(((d > z) & (z == 0)) | ((d < z) & (z == m - 1)))
        def _():
            for h in range(BANDS):
                hop(s, cc, h).start()

    def combine(s, cc, h, pos):
        d = owner(s)
        at = rows_of(h)

        @pl.when(((d > z) & (z == pos)) | ((d < z) & (m - 1 - z == pos)))
        def _():
            rcopy(part.at[s, cc, at], come.at[s, cc, at], gs.at[s, cc, h], gr.at[s, cc, h], partner).wait_recv()
            part[s, cc, at] = (part[s, cc, at].astype(F32) + come[s, cc, at].astype(F32)).astype(BF16)
            hop(s, cc, h).start()

    def combine_own(pos):
        @pl.loop(0, 2 * BANDS)
        def _(i):
            combine(0, i // BANDS, i % BANDS, pos)

    def combine_near(cc, pos):
        @pl.loop(0, BANDS * (n - 2))
        def _(i):
            k = i // BANDS
            combine(1 + k + k // (half - 1), cc, i % BANDS, pos)

    local[0].wait()
    local[1].wait()
    product(0, 0, 0)
    rcopy(pieces, wbuf.at[1, 0], os.at[0], orr.at[0], partner).wait_recv()
    product(0, 1, 0)

    pl.semaphore_signal(cred.at[0], inc=1, device_id=to_left, device_id_type=MESH)
    pl.semaphore_signal(cred.at[1], inc=1, device_id=to_right, device_id_type=MESH)
    pl.semaphore_signal(cred.at[2], inc=1, device_id=partner, device_id_type=MESH)
    for copy in local[2:]:
        copy.wait()
    for k in range(3):
        pl.semaphore_wait(cred.at[k], 1)

    mid = PIECES // 2

    def arrived(stage, way, i, ph):
        rcopy(wbuf.at[0, ph, i], wbuf.at[0, ph, i], ws.at[stage, way, i], wr.at[stage, way, i], partner).wait_recv()

    def across(s, i):
        start(rcopy(wbuf.at[0, phys(s), i], wbuf.at[1, phys(s), i], ds.at[s, i], dr.at[s, i], partner))

    def relay(stage, i):
        last = stage == half - 2
        for way in range(2):
            q = i if way == 0 else PIECES - 1 - i
            s = stage + 1 if way == 0 else n - stage - 1
            arrived(stage, way, q, phys(s))
            on = stage + 2 if way == 0 else n - stage - 2
            if not last or i < mid:
                start(rcopy(wbuf.at[0, phys(s), q], wbuf.at[0, phys(on), q], ws.at[stage + 1, way, q],
                            wr.at[stage + 1, way, q], to_right if way == 0 else to_left))
            across(s, q)
        if last and i == mid:
            ph = phys(half - 1) * (1 - c) + phys(half + 1) * c
            start(rcopy(wbuf.at[0, ph, mid], wbuf.at[0, 0, mid], ws.at[half - 1, 0, mid], wr.at[half - 1, 0, mid],
                        (right * (1 - c) + left * c, z, c)))

    for stage in range(half - 2):
        for i in range(PIECES):
            relay(stage, i)
    for i in range(mid):
        relay(half - 2, i)

    for way, j, t, there in sides:
        for kind, dst in enumerate((dnv, upv)):
            block = dst.at[pl.ds(t * own, own), mine]
            pl.when(there)(rcopy(
                block, block, as_.at[way, j - 1, kind], ar.at[way, j - 1, kind], partner).wait_recv)
            start(rcopy(block, block, xs.at[way, j - 1, kind], xr.at[way, j - 1, kind], partner), there)
    for way, j, t, there in sides:
        for kind, dst in enumerate((dnv, upv)):
            block = dst.at[pl.ds(t * own, own), others]
            pl.when(there)(rcopy(
                block, block, xs.at[way, j - 1, kind], xr.at[way, j - 1, kind], partner).wait_recv)

    @pl.loop(0, blocks)
    def _(b):
        t = tenants_of[b]
        at = pl.ds(pl.multiple_of(b * BLOCK, BLOCK), BLOCK)
        down_t, up_t = dnv[t], upv[t]
        first = nt(tokv[at, :], jnp.concatenate([down_t, jnp.zeros_like(down_t)], axis=0))
        second = nt(cotv[at, :], jnp.concatenate([jnp.zeros_like(up_t), up_t], axis=0))
        sums[z, at, :] = first + second

    for j in range(1, m):
        t = (z + j) % m
        start(rcopy(sums.at[z], sums.at[z], ss.at[j - 1], sr.at[z], plane(t)))
    first_hop(0, 0)
    first_hop(0, 1)

    def pass_tokens(k):
        for way, t, there in ((0, z - k, z - k >= 0), (1, z + k, z + k < m)):
            nxt = z + 1 if way == 0 else z - 1
            more = there & ((nxt < m) if way == 0 else (nxt >= 0))
            for ca in range(2):
                pl.when(there)(rcopy(
                    tv.at[t, ca], tv.at[t, ca], ts.at[0, 0, ca], tr.at[t, ca], partner).wait_recv)
                if k < m - 1:
                    start(rcopy(tv.at[t, ca], tv.at[t, ca], ts.at[k, way, ca], tr.at[t, ca], plane(nxt)), more)

    relay(half - 2, mid)
    pass_tokens(1)
    for i in range(mid + 1, PIECES):
        relay(half - 2, i)

    combine_own(1)
    for i in range(n - 2):
        s = 1 + i + i // (half - 1)
        for q in range(PIECES):
            rcopy(wbuf.at[1, phys(s), q], wbuf.at[1, phys(s), q], ds.at[s, q], dr.at[s, q], partner).wait_recv()

    @pl.loop(0, 2 * (n - 2))
    def _(i):
        k = i % (n - 2)
        product(1 + k + k // (half - 1), i // (n - 2), 1 + k)
        first_hop(1 + k + k // (half - 1), i // (n - 2))

    for j in range(1, m):
        t = (z + j) % m
        rcopy(sums.at[t], sums.at[t], ss.at[j - 1], sr.at[t], partner).wait_recv()

    @pl.loop(0, blocks)
    def _(b):
        t = tenants_of[b]
        r = ranks[t]
        at = pl.ds(pl.multiple_of(b * BLOCK, BLOCK), BLOCK)
        total = sums[0, at, :]
        for k in range(1, m):
            total = total + sums[k, at, :]
        lane = lax.broadcasted_iota(jnp.int32, total.shape, 1)
        slot = jnp.where(lane >= rank, lane - rank, lane)
        width = jnp.full(total.shape, r, jnp.int32).astype(F32)
        gain = jnp.where(slot < r, alpha_scale / width, 0.0)
        scaled = (total * gain).astype(BF16)
        column = lax.broadcasted_iota(jnp.int32, (BLOCK, tenants * rank), 1)
        chosen = (column >= t * rank) & (column < (t + 1) * rank)
        ada[at, :] = jnp.where(chosen, nn(scaled, eye[0]), 0.0).astype(BF16)
        adg[at, :] = jnp.where(chosen, nn(scaled, eye[1]), 0.0).astype(BF16)

    tall = gp.shape[0]

    def grads(core, other):
        lanes = pl.ds(pl.multiple_of(core * tall, 128), tall)

        @pl.loop(0, lf // tile)
        def _(j):
            columns = pl.ds(pl.multiple_of(j * tile, tile), tile)
            term = tn(ada[:, lanes], cotv[:, columns])
            if other is not None:
                term = term + other[:, columns].astype(F32)
            gp[:, columns] = term.astype(BF16)

        term = tn(adg[:, lanes], tokv[...])
        if other is not None:
            term = term + other[:, lf:].astype(F32)
        gp[:, lf:] = term.astype(BF16)

    grads(1 - c, None)
    swap = rcopy(gp, dpr, ps.at[0], pr.at[0], partner)
    swap.start()
    for k in range(2, m - 1):
        pass_tokens(k)
    swap.wait()
    grads(c, dpr)
    for pos in range(2, m - 1):
        combine_own(pos)
    combine_near(0, 1)

    def far(i):
        for way in range(2):
            q = i if way == 0 else PIECES - 1 - i
            arrived(half - 1, way, q, 0)
            across(half, q)

    def forward(spots, body, first=0, last=lf // tile):
        @pl.loop(first, last)
        def _(j):
            columns = pl.ds(pl.multiple_of(j * tile, tile), tile)
            total = None
            for s, cc, ph in spots:
                block = wbuf[ph[0], ph[1], :, :, columns].reshape(depth, tile)
                term = nn(tv[owner(s), c if cc == 0 else 1 - c], block)
                total = term if total is None else total + term
            body(columns, total)

    def set_hid(columns, total):
        hid[:, columns] = total

    def add_hid(columns, total):
        hid[:, columns] += total

    if n == 4:
        d_first, d_last = owner(1), owner(n - 1)
        later = ((d_first - z) * (d_first - z) > (d_last - z) * (d_last - z)).astype(jnp.int32)
        turns = (later, 1 - later)
    else:
        pass_tokens(m - 1)
        turns = range(n - 2)
    for i, k in enumerate(turns):
        s = 1 + k + k // (half - 1)
        forward(((s, 0, (0, 1 + k)), (s, 1, (1, 1 + k))), add_hid if i else set_hid)
        if n == 4 and i == 0:
            pass_tokens(m - 1)
            far(0)
    if n != 4:
        far(0)

    across_dev = snake((place + half) % n, n)
    hq = quarter // 2
    merged = n == 4

    def rows_at(dev, h):
        return pl.ds(pl.multiple_of(dev * quarter + h * hq, 16), hq)

    def half_at(h):
        return pl.ds(h * hq, hq)

    parts = ((slice(0, lf), gu_o), (slice(lf, lf + ld), gd_o))

    def share_to(i, dev, h, slot, target):
        lanes = parts[i][0]
        return rcopy(gp.at[rows_at(dev, h), lanes], rsr.at[slot, half_at(h), lanes], rs.at[slot, h, i],
                     rr.at[slot, h, i], target)

    def share_from(i, slot, h):
        there = rsr.at[slot, half_at(h), parts[i][0]]
        rcopy(there, there, rs.at[slot, h, i], rr.at[slot, h, i], partner).wait_recv()

    for i in range(2):
        if merged:
            start(share_to(i, across_dev, 0, 0, to_right))
            start(share_to(i, across_dev, 1, 0, to_left))
            start(share_to(i, right, 1, 1, to_right))
            start(share_to(i, left, 0, 2, to_left))
        else:
            for k in range(1, n):
                peer = snake((place + k) % n, n)
                for h in range(2):
                    start(share_to(i, peer, h, k - 1, (peer, z, c)))

    rcopy(pieces, pair_o, os.at[1], orr.at[1], partner).wait_recv()
    again = [pltpu.make_async_copy(pieces, wbuf.at[1, 1], l_sem.at[0]),
             pltpu.make_async_copy(pair_o, wbuf.at[1, 2], l_sem.at[1])]
    for copy in again:
        copy.start()
    combine_near(1, 1)

    for i in range(1, mid):
        far(i)
    arrived(half - 1, 0, mid, 0)
    across(half, mid)
    product(half, 0, 0)
    first_hop(half, 0)
    for q in range(PIECES):
        rcopy(wbuf.at[1, 0, q], wbuf.at[1, 0, q], ds.at[half, q], dr.at[half, q], partner).wait_recv()
    product(half, 1, 0)
    first_hop(half, 1)
    def strips(i, body):
        lanes = parts[i][0]
        strip = tile_of(lanes.stop - lanes.start, 256)

        @pl.loop(0, (lanes.stop - lanes.start) // strip)
        def _(j):
            body(pl.ds(pl.multiple_of(lanes.start + j * strip, 128), strip))

    def merge(i):
        for h, dev, slot, target in ((0, right, 1, to_right), (1, left, 2, to_left)):
            share_from(i, 0, h)
            at = rows_at(dev, h)

            def add(columns):
                total = gp[at, columns].astype(F32) + rsr[0, h * hq:(h + 1) * hq, columns].astype(F32)
                gp[at, columns] = total.astype(BF16)

            strips(i, add)
            start(share_to(i, dev, h, slot, target))

    if merged:
        merge(0)
    for pos in range(2, m - 1):
        combine_near(0, pos)
        combine_near(1, pos)

    coming = sorted(
        (BANDS * cc + h + 2 * pos, pos, cc, h) for cc in range(2) for h in range(BANDS) for pos in range(1, m - 1))

    def combine_next(count):
        for _, pos, cc, h in coming[:count]:
            combine(half, cc, h, pos)
        del coming[:count]

    combine_next(2)
    if merged:
        merge(1)
    for copy in again:
        copy.wait()
    forward(((0, 0, (1, 1)), (0, 1, (1, 2))), add_hid)
    combine_next(4)

    slots = range(1 if merged else 0, n - 1)
    keep = []

    def result_to(i, dev, h, slot, target, own_rows):
        lanes, dst = parts[i]
        there = dst.at[dev, half_at(h)]
        start(rcopy(ags.at[half_at(h), lanes] if own_rows else there, there, qs.at[slot, h, i], qr.at[slot, h, i],
                    target))

    def result_from(i, dev, h, slot):
        there = parts[i][1].at[dev, half_at(h)]
        rcopy(there, there, qs.at[slot, h, i], qr.at[slot, h, i], partner).wait_recv()

    def result(i):
        for slot in slots:
            for h in range(2):
                share_from(i, slot, h)

        def add(columns):
            total = gp[pl.ds(pl.multiple_of(f * quarter, 16), quarter), columns].astype(F32)
            for slot in slots:
                total = total + rsr[slot, :, columns].astype(F32)
            ags[:, columns] = total.astype(BF16)

        strips(i, add)
        if merged:
            for first in range(2):
                result_to(i, f, first, 0, to_right, True)
                result_to(i, f, 1 - first, 1, to_left, True)
        else:
            for k in range(1, n):
                for h in range(2):
                    result_to(i, f, h, k - 1, (snake((place + k) % n, n), z, c), True)
        lanes, dst = parts[i]
        keep.append(pltpu.make_async_copy(ags.at[:, lanes], dst.at[f], o_sem.at[i]))
        keep[-1].start()

    def result_on(i):
        if merged:
            result_from(i, left, 0, 0)
            result_to(i, left, 0, 2, to_right, False)
            result_from(i, right, 1, 1)
            result_to(i, right, 1, 2, to_left, False)

    result(0)
    result(1)
    combine_next(6)
    result_on(0)

    up_flat = tenants * rank
    farthest = ((half, 0, (0, 0)), (half, 1, (1, 0)))
    early = lf // tile // 2

    def finish(columns, total):
        total = total + nn(ada[...], upv[:, :, columns].reshape(up_flat, tile))
        cotv[:, columns] = (hid[:, columns] + total).astype(BF16)

    combine_next(2)
    forward(farthest, finish, 0, early)
    combine_next(len(coming))
    result_on(1)

    forward(farthest, finish, early)
    hidden = pltpu.make_async_copy(cotv, hid_o, o_sem.at[2])
    hidden.start()

    s_z = (place + n - snake(z, n)) % n
    for slots, cond in (((n,), z == 0), ((s_z,), z == m - 1), ((s_z, n), (z > 0) & (z < m - 1))):
        @pl.when(cond)
        def _():
            for slot in slots:
                for cc in range(2):
                    for h in range(BANDS):
                        at = rows_of(h)
                        rcopy(come.at[slot, cc, at], come.at[slot, cc, at], gs.at[0, cc, h], gr.at[slot, cc, h],
                              partner).wait_recv()
            term = nn(adg[...], dnv[...].reshape(up_flat, ld))
            for ca in range(2):
                cc = ca + c - 2 * ca * c
                total = term[:, ca * depth:(ca + 1) * depth] + part[s_z, cc].astype(F32)
                for slot in slots:
                    total = total + come[slot, cc].astype(F32)
                tokv[:, ca * depth:(ca + 1) * depth] = total.astype(BF16)

    back = pltpu.make_async_copy(tokv, gt_o, o_sem.at[3])
    back.start()

    for i in range(2):
        if merged:
            for dev, h, slot in ((left, 1, 0), (right, 0, 1), (across_dev, 0, 2), (across_dev, 1, 2)):
                result_from(i, dev, h, slot)
        else:
            for k in range(1, n):
                for h in range(2):
                    result_from(i, snake((place + n - k) % n, n), h, k - 1)
    for cond, copy in sent:
        if cond is None:
            copy.wait_send()
        else:
            pl.when(cond)(copy.wait_send)
    for s in range(n):
        for cc in range(2):
            for h in range(BANDS):
                pl.when(owner(s) != z)(hop(s, cc, h).wait_send)
    for copy in keep:
        copy.wait()
    hidden.wait()
    back.wait()


def make_shards(mesh):
    n, m, dp_n = mesh.shape["fsdp"], mesh.shape["tenant"], mesh.shape["dp"]
    assert dp_n == 2 and n == m and n % 2 == 0 and n >= 4

    def shards(tokens, block_tenant_index, ranks, frozen_up_weight, tenant_down_adapters,
               tenant_up_adapters, cotangent):
        rows, ld = tokens.shape
        lf = cotangent.shape[1]
        tenants = ranks.shape[0]
        rank = tenant_down_adapters.shape[1]
        depth = frozen_up_weight.shape[0]
        piece = depth // PIECES
        tall = tenants * rank // dp_n
        quarter = tall // n
        half = n // 2
        split = tokens
        if depth % 128:
            split = tokens.reshape(rows, ld // depth, depth).transpose(1, 0, 2)
        eye = np.zeros((2, 2 * rank, tenants * rank), np.float32)
        for t in range(tenants):
            for k in range(2):
                eye[k, k * rank:(k + 1) * rank, t * rank:(t + 1) * rank] = np.eye(rank)

        any_space = pl.BlockSpec(memory_space=pl.ANY)
        dma = pltpu.SemaphoreType.DMA
        hidden, back, grad_up, grad_down, _ = pl.pallas_call(
            functools.partial(kernel, n, m),
            out_shape=(
                jax.ShapeDtypeStruct((rows, lf), BF16),
                jax.ShapeDtypeStruct((rows, ld), BF16),
                jax.ShapeDtypeStruct((n, quarter, lf), BF16),
                jax.ShapeDtypeStruct((n, quarter, ld), BF16),
                jax.ShapeDtypeStruct((PIECES, piece, lf), BF16),
            ),
            in_specs=[pl.BlockSpec(memory_space=pltpu.SMEM)] * 2 + [any_space] * 7,
            out_specs=(any_space,) * 5,
            scratch_shapes=[
                pltpu.VMEM((2, n - 1, PIECES, piece, lf), BF16),
                pltpu.VMEM((rows, lf), BF16),
                pltpu.VMEM((rows, ld), BF16),
                pltpu.VMEM((m, 2, rows, depth), BF16),
                pltpu.VMEM((rows, lf), F32),
                pltpu.VMEM((tenants, rank, lf), BF16),
                pltpu.VMEM((tenants, rank, ld), BF16),
                pltpu.VMEM((n, 2, rows, depth), BF16),
                pltpu.VMEM((n + 1, 2, rows, depth), BF16),
                pltpu.VMEM((tall, lf + ld), BF16),
                pltpu.VMEM((tall, lf + ld), BF16),
                pltpu.VMEM((n - 1, quarter, lf + ld), BF16),
                pltpu.VMEM((quarter, lf + ld), BF16),
                pltpu.VMEM((m, rows, 2 * rank), F32),
                pltpu.VMEM((rows, tenants * rank), BF16),
                pltpu.VMEM((rows, tenants * rank), BF16),
                pltpu.VMEM(eye.shape, BF16),
                dma((8,)),
                dma((half, 2, PIECES)), dma((half, 2, PIECES)),
                dma((2,)), dma((2,)),
                dma((n, PIECES)), dma((n, PIECES)),
                dma((m - 1, 2, 2)), dma((m, 2)),
                dma((2, m - 1, 2)), dma((2, m - 1, 2)),
                dma((2, m - 1, 2)), dma((2, m - 1, 2)),
                dma((m - 1,)), dma((m,)),
                dma((n, 2, BANDS)), dma((n + 1, 2, BANDS)),
                dma((1,)), dma((1,)),
                dma((n - 1, 2, 2)), dma((n - 1, 2, 2)),
                dma((n - 1, 2, 2)), dma((n - 1, 2, 2)),
                dma((4,)),
                pltpu.SemaphoreType.REGULAR((3,)),
            ],
            compiler_params=pltpu.CompilerParams(
                collective_id=0, has_side_effects=True, vmem_limit_bytes=67043328
            ),
        )(block_tenant_index, ranks, tokens, split, cotangent, frozen_up_weight,
          tenant_down_adapters, tenant_up_adapters, jnp.asarray(eye, BF16))
        results = (hidden, back, grad_up, grad_down)
        hidden, back, grad_up, grad_down = pl.pallas_call(
            finish_kernel,
            out_shape=tuple(
                jax.ShapeDtypeStruct(x.shape, F32 if x.ndim == 3 else BF16) for x in results
            ),
            in_specs=[any_space] * 4,
            out_specs=(any_space,) * 4,
            scratch_shapes=[pltpu.VMEM(x.shape, BF16) for x in results]
            + [pltpu.VMEM(x.shape, F32) for x in results[2:]]
            + [dma((n + 3,)), dma((n + 3,))],
            compiler_params=pltpu.CompilerParams(vmem_limit_bytes=67043328),
        )(*results)
        grad_up = grad_up.reshape(tenants // dp_n, rank, lf)
        grad_down = grad_down.reshape(tenants // dp_n, rank, ld)
        return (hidden, back, grad_down, grad_up)

    return shards


def solution(mesh):
    return jax.shard_map(
        make_shards(mesh),
        mesh=mesh,
        in_specs=(
            P(("fsdp", "dp"), "tenant"),
            P(("fsdp", "dp")),
            P(),
            P(("fsdp", "dp"), "tenant"),
            P("tenant", None, None),
            P("tenant", None, None),
            P(("fsdp", "dp"), "tenant"),
        ),
        out_specs=(
            P(("fsdp", "dp"), "tenant"),
            P(("fsdp", "dp"), "tenant"),
            P("dp", None, "tenant"),
            P("dp", None, "tenant"),
        ),
        check_vma=False,
    )
```
